32 devices in a mesh: gx: 4 (over y, x), gy: 2 (over core), gz: 4 (over z).
Axes of the slice: x: 2, y: 2, z: 4, core: 2. Of those that a mesh axis runs over, the one named last changes fastest.
Arguments:
- pair: bfloat16 [128, 1024, 1024], P('gz', 'gy', 'gx'), may hold values from -6 to 6
- pair_mask: int32 [1024, 1024], P('gy', 'gx'), may hold values 0 or 1
- in_gain: float32 [128], replicated, may hold values from 0.5 to 2
- w_left: bfloat16 [128, 128], P(None, 'gz'), may hold values from -0.5 to 0.5
- w_left_gate: bfloat16 [128, 128], P(None, 'gz'), may hold values from -0.5 to 0.5
- w_right: bfloat16 [128, 128], P(None, 'gz'), may hold values from -0.5 to 0.5
- w_right_gate: bfloat16 [128, 128], P(None, 'gz'), may hold values from -0.5 to 0.5
- w_out_gate: bfloat16 [128, 128], P(None, 'gz'), may hold values from -0.5 to 0.5
- out_gain: float32 [128], P('gz'), may hold values from 0.5 to 2
- w_out: bfloat16 [128, 128], P(None, 'gz'), may hold values from -0.5 to 0.5
Outputs:
- update: bfloat16 [128, 1024, 1024], P('gz', 'gy', 'gx')
The draws below stay inside these ranges and needn't reach their ends.
All inputs are finite; a program needn't handle non-finite values. No bound on the sum of `pair_mask` on one device may be relied on, other than what follows from the above.
Results may differ from the reference program's by a relative error of at most 0.0078.
Values may be sent and summed in bfloat16 or wider, within the bound.
No kernel may reach another device: no remote copies, remote signals or barrier semaphores. Data moves between devices by JAX's collectives and lax.ppermute only.
A program may use at most 192 MiB of HBM per device.

```python
import math
import jax
import jax.numpy as jnp
from jax import lax

CZ = 128
CH = 128
N = 1024


def set_ends(values, own_key, smallest, high):
    longest = values.shape.index(max(values.shape))
    spots = []
    for shift in (0, 1):
        where = [jax.random.randint(jax.random.fold_in(own_key, axis), (), 0, length) for axis, length in enumerate(values.shape)]
        where[longest] = (where[longest] + shift) % values.shape[longest]
        spots.append(tuple(where))
    return values.at[spots[0]].set(smallest).at[spots[1]].set(high)


def block_levels(own_key, shape, shards, least, top_value):
    level, own = 1.0, jax.random.fold_in(own_key, 6)
    for dim, shards_of in shards:
        steps = jnp.exp(jax.random.uniform(jax.random.fold_in(own, dim), (shards_of,), jnp.float32, least / len(shards), top_value / len(shards)))
        level = level * jnp.repeat(steps, shape[dim] // shards_of).reshape([-1 if axis == dim else 1 for axis in range(len(shape))])
    return level


def normal_values(key, dims, deviation, bound, cuts=(), held_as=jnp.bfloat16):
    entries = jax.random.normal(key, dims, jnp.float32) * deviation
    if len(cuts) > 0:
        entries = block_levels(key, dims, cuts, -0.22, 0.18) * entries
    return jnp.clip(entries, min=-bound, max=bound).astype(held_as)


def setup_inputs(seed: int = 0) -> dict:
    arg_keys = jax.random.split(jax.random.key(seed), 11)
    pair = normal_values(arg_keys[0], (CZ, N, N), 1.0, 6.0, ((0, 4), (1, 2), (2, 4)))
    pair_mask = set_ends((jax.random.randint(arg_keys[1], (N, N), 0, 8) < 7).astype(jnp.int32), jax.random.fold_in(arg_keys[1], 1), 0, 1)
    in_gain = jnp.clip(jnp.exp(jax.random.uniform(arg_keys[2], (CZ,), jnp.float32, math.log(0.5), math.log(2.0))), 0.5, 2.0)
    w_left = normal_values(arg_keys[3], (CZ, CH), CZ ** -0.5, 0.5, ((1, 4),))
    w_left_gate = normal_values(arg_keys[4], (CZ, CH), CZ ** -0.5, 0.5, ((1, 4),))
    w_right = normal_values(arg_keys[5], (CZ, CH), CZ ** -0.5, 0.5, ((1, 4),))
    w_right_gate = normal_values(arg_keys[6], (CZ, CH), CZ ** -0.5, 0.5, ((1, 4),))
    w_out_gate = normal_values(arg_keys[7], (CZ, CZ), CZ ** -0.5, 0.5, ((1, 4),))
    out_gain = jnp.clip(jnp.exp(math.log(2.0) - 1.3862944 * jax.random.uniform(arg_keys[8], (CH,), jnp.float32) ** block_levels(arg_keys[8], (CH,), ((0, 4),), -0.2, 0.2)), 0.5, 2.0)
    w_out = normal_values(arg_keys[9], (CH, CZ), CH ** -0.5, 0.5, ((1, 4),))
    return {"pair": pair, "pair_mask": pair_mask, "in_gain": in_gain, "w_left": w_left, "w_left_gate": w_left_gate, "w_right": w_right, "w_right_gate": w_right_gate, "w_out_gate": w_out_gate, "out_gain": out_gain, "w_out": w_out}


epsilon = 1e-05

def layer_norm(values, gain):
    average = lax.optimization_barrier(jnp.mean(values, axis=0))
    centered = values - average
    spread = lax.optimization_barrier(jnp.mean(jnp.square(centered), axis=0))
    return centered * lax.rsqrt(spread + epsilon) * gain[:, None, None]

def reference(pair, pair_mask, in_gain, w_left, w_left_gate, w_right, w_right_gate, w_out_gate, out_gain, w_out):
    normed = layer_norm(pair.astype(jnp.float32), in_gain).astype(jnp.bfloat16)
    normed_f = normed.astype(jnp.float32)
    mask_float = pair_mask.astype(jnp.float32)[None]

    def project(weight):
        return jnp.einsum('cik,ch->hik', normed_f, weight.astype(jnp.float32))
    left_rows = (mask_float * jax.nn.sigmoid(project(w_left_gate)) * project(w_left)).astype(jnp.bfloat16)
    right_rows = (mask_float * jax.nn.sigmoid(project(w_right_gate)) * project(w_right)).astype(jnp.bfloat16)

    def channel_product(operands):
        return jnp.dot(operands[0], operands[1].T, preferred_element_type=jnp.float32)
    mixed_sum = lax.map(channel_product, (left_rows, right_rows))
    normed_mix = layer_norm(mixed_sum, out_gain).astype(jnp.bfloat16)
    out_gate = jax.nn.sigmoid(jnp.einsum('cij,cd->dij', normed_f, w_out_gate.astype(jnp.float32)))
    projected = jnp.einsum('hij,hd->dij', normed_mix.astype(jnp.float32), w_out.astype(jnp.float32))
    return (out_gate * projected).astype(jnp.bfloat16)
```

```python
import functools

import jax
import jax.numpy as jnp
from jax import lax
from jax.experimental import pallas as pl
from jax.experimental.pallas import tpu as pltpu
from jax.sharding import PartitionSpec as P

epsilon = 1e-05
CHUNKS = 4
ROWS = 16
LANES = 128
F32, BF16 = jnp.float32, jnp.bfloat16
ARBITRARY = pltpu.GridDimensionSemantics.ARBITRARY

ROW_ORDER = ((0, 1, 2, 3), (1, 0, 2, 3), (2, 3, 1, 0), (3, 2, 1, 0))
COL_ORDER = ((0, 1, 2, 3), (1, 2, 3, 0), (2, 1, 0, 3), (3, 2, 1, 0))


def sigmoid(x):
    return 1.0 / (1.0 + jnp.exp(-x))


def norm_channels(x, gain):
    average = jnp.mean(x, axis=0, keepdims=True)
    centered = x - average
    spread = jnp.mean(jnp.square(centered), axis=0, keepdims=True)
    return (centered * lax.rsqrt(spread + epsilon) * gain).astype(BF16)


def dot(a, b, dims=(((1,), (0,)), ((), ()))):
    return lax.dot_general(a, b, dims, preferred_element_type=F32)


def project_kernel(slots, emit, parts, plane_ref, *refs):
    n_in = sum(len(slot) for slot in slots)
    ins = refs[:n_in]
    mask_ref, weight_ref, gain_ref = refs[n_in : n_in + 3]
    outs = refs[n_in + 3 : n_in + 3 + parts + (1 if emit else 0)]
    x_ref, y_ref = refs[-2:]
    plane = plane_ref[0]
    width = ins[0].shape[-1]
    halves = width // LANES
    channels = ins[0].shape[0]
    position = 0
    for slot_index, slot in enumerate(slots):
        base = slot_index * channels * ROWS
        for planes in slot:
            source = ins[position]
            position += 1
            hit = functools.reduce(jnp.logical_or, [plane == p for p in planes])

            @pl.when(hit)
            def _(source=source, base=base):
                for half in range(halves):
                    block = source[:, 0, :, half * LANES : (half + 1) * LANES].astype(F32)
                    x_ref[half, pl.ds(base, channels * ROWS), :] = block.reshape(channels * ROWS, LANES)

    total = len(slots) * channels
    hidden = weight_ref.shape[0] // 2
    gain = gain_ref[...]

    def step(row, carry):
        normed = [
            norm_channels(x_ref[half, pl.ds(row, total, stride=ROWS), :], gain) for half in range(halves)
        ]
        if emit:
            upper = (plane >> 1) == 1
            chosen = jnp.where(upper, normed[1].astype(F32), normed[0].astype(F32))
            outs[parts][0, row] = chosen.astype(BF16)
        both = dot(weight_ref[...], jnp.concatenate(normed, axis=1))
        mask = mask_ref[0, pl.ds(row, 1), :]
        value = mask * sigmoid(both[:hidden]) * both[hidden:]
        for half in range(halves):
            y_ref[half, pl.ds(row, hidden, stride=ROWS), :] = value[:, half * LANES : (half + 1) * LANES]
        return carry

    lax.fori_loop(0, ROWS, step, 0)
    part = hidden // parts
    for m in range(parts):
        for half in range(halves):
            block = y_ref[half, pl.ds(m * part * ROWS, part * ROWS), :].reshape(part, ROWS, LANES)
            outs[m][:, 0, :, half * LANES : (half + 1) * LANES] = block.astype(BF16)


def project(plane, slots, arrays, mask, weight, gain, parts, emit):
    channels, blocks, size, width = arrays[0].shape
    hidden = weight.shape[0] // 2
    total = len(slots) * channels
    planes = tuple(tuple(p for _, p in slot) for slot in slots)
    ins = [arrays[index] for slot in slots for index, _ in slot]
    block = pl.BlockSpec((channels, 1, ROWS, width), lambda n, t: (0, n, t, 0))
    whole = lambda n, t: (0, 0)
    out_specs = [pl.BlockSpec((hidden // parts, 1, ROWS, width), lambda n, t: (0, n, t, 0))] * parts
    out_shape = [jax.ShapeDtypeStruct((hidden // parts, blocks, size, width), BF16)] * parts
    if emit:
        out_specs = out_specs + [pl.BlockSpec((1, ROWS, total, LANES), lambda n, t: (n, t, 0, 0))]
        out_shape = out_shape + [jax.ShapeDtypeStruct((blocks, size, total, LANES), BF16)]
    pixels = blocks * size * width
    return pl.pallas_call(
        functools.partial(project_kernel, planes, emit, parts),
        grid=(blocks, size // ROWS),
        in_specs=[pl.BlockSpec(memory_space=pltpu.SMEM)]
        + [block] * len(ins)
        + [
            pl.BlockSpec((1, ROWS, width), lambda n, t: (n, t, 0)),
            pl.BlockSpec(weight.shape, whole),
            pl.BlockSpec(gain.shape, whole),
        ],
        out_specs=out_specs,
        out_shape=out_shape,
        scratch_shapes=[
            pltpu.VMEM((width // LANES, total * ROWS, LANES), F32),
            pltpu.VMEM((width // LANES, hidden * ROWS, LANES), F32),
        ],
        compiler_params=pltpu.CompilerParams(dimension_semantics=(ARBITRARY, ARBITRARY)),
        cost_estimate=pl.CostEstimate(
            flops=16 * pixels * total * hidden, bytes_accessed=2 * pixels * (total * 3 + hidden), transcendentals=0
        ),
        name="project",
    )(plane, *ins, mask, weight, gain)


def product_kernel(parts, chunks, flags_ref, *refs):
    lefts = refs[:parts]
    rights = refs[parts : parts + 2 * chunks * parts]
    outs = refs[parts + 2 * chunks * parts :]
    heads, blocks, size, width = lefts[0].shape
    for head in range(heads):
        left = jnp.concatenate([ref[head].reshape(blocks * size, width) for ref in lefts], axis=1)
        rows = []
        for core in range(2):
            for n in range(blocks):
                for g in range(chunks):
                    pieces = [rights[(core * chunks + g) * parts + m][head, n] for m in range(parts)]
                    rows.append(jnp.concatenate(pieces, axis=1))
        right = jnp.concatenate(rows, axis=0)
        mixed = dot(left, right, (((1,), (1,)), ((), ())))
        span = right.shape[0] // (2 * blocks)
        pieces = [mixed[:, p * span : (p + 1) * span] for p in range(2 * blocks)]
        for m in range(parts):
            pick = flags_ref[m]
            value = pieces[0]
            for p in range(1, len(pieces)):
                value = jnp.where(pick == p, pieces[p], value)
            outs[m][head] = value.astype(BF16).reshape(blocks, size, span)


def product(flags, lefts, rights, heads):
    parts = len(lefts)
    hidden, blocks, size, width = lefts[0].shape
    chunks = len(rights) // (2 * parts)
    span = chunks * size
    block = pl.BlockSpec((heads, blocks, size, width), lambda h: (h, 0, 0, 0))
    rows = blocks * size
    return pl.pallas_call(
        functools.partial(product_kernel, parts, chunks),
        grid=(hidden // heads,),
        in_specs=[pl.BlockSpec(memory_space=pltpu.SMEM)] + [block] * (len(lefts) + len(rights)),
        out_specs=[pl.BlockSpec((heads, blocks, size, span), lambda h: (h, 0, 0, 0))] * parts,
        out_shape=[jax.ShapeDtypeStruct((hidden, blocks, size, span), BF16)] * parts,
        compiler_params=pltpu.CompilerParams(dimension_semantics=(ARBITRARY,)),
        cost_estimate=pl.CostEstimate(
            flops=2 * hidden * rows * (2 * blocks * span) * width * parts,
            bytes_accessed=2 * hidden * width * parts * (rows + 2 * blocks * span),
            transcendentals=0,
        ),
        name="product",
    )(flags, *lefts, *rights)


def finish_kernel(parts, *refs):
    mixed = refs[:parts]
    normed_ref, out_ref, gate_ref, gain_ref = refs[parts : parts + 4]
    outs = refs[parts + 4 : -2]
    x_ref, y_ref = refs[-2:]
    part = mixed[0].shape[0]
    for m in range(parts):
        x_ref[pl.ds(m * part * ROWS, part * ROWS), :] = mixed[m][:, 0].astype(F32).reshape(part * ROWS, LANES)
    total = parts * part
    gain = gain_ref[...]
    together = 2

    def step(pair, carry):
        base = pair * together
        normed = [
            norm_channels(x_ref[pl.ds(base + r, total, stride=ROWS), :], gain) for r in range(together)
        ]
        gates = dot(gate_ref[...], jnp.concatenate([normed_ref[0, base + r] for r in range(together)], axis=1))
        value = sigmoid(gates) * dot(out_ref[...], jnp.concatenate(normed, axis=1))
        for r in range(together):
            y_ref[pl.ds(base + r, value.shape[0], stride=ROWS), :] = value[:, r * LANES : (r + 1) * LANES]
        return carry

    lax.fori_loop(0, ROWS // together, step, 0)
    part = out_ref.shape[0] // len(outs)
    for q, out in enumerate(outs):
        block = y_ref[pl.ds(q * part * ROWS, part * ROWS), :].reshape(part, ROWS, LANES)
        out[:, 0] = block.astype(BF16)


def finish(mixed, normed, w_out, w_gate, gain, planes):
    part, blocks, size, width = mixed[0].shape
    depth = w_out.shape[0]
    total = part * len(mixed)
    whole = lambda n, t: (0, 0)
    pixels = blocks * size * width
    return pl.pallas_call(
        functools.partial(finish_kernel, len(mixed)),
        grid=(blocks, size // ROWS),
        in_specs=[pl.BlockSpec((part, 1, ROWS, width), lambda n, t: (0, n, t, 0))] * len(mixed)
        + [
            pl.BlockSpec((1, ROWS, normed.shape[2], width), lambda n, t: (n, t, 0, 0)),
            pl.BlockSpec(w_out.shape, whole),
            pl.BlockSpec(w_gate.shape, whole),
            pl.BlockSpec(gain.shape, whole),
        ],
        out_specs=[pl.BlockSpec((depth // planes, 1, ROWS, width), lambda n, t: (0, n, t, 0))] * planes,
        out_shape=[jax.ShapeDtypeStruct((depth // planes, blocks, size, width), BF16)] * planes,
        scratch_shapes=[pltpu.VMEM((total * ROWS, width), F32), pltpu.VMEM((depth * ROWS, width), F32)],
        compiler_params=pltpu.CompilerParams(dimension_semantics=(ARBITRARY, ARBITRARY)),
        cost_estimate=pl.CostEstimate(
            flops=16 * pixels * total * depth, bytes_accessed=2 * pixels * total * 3, transcendentals=0
        ),
        name="finish",
    )(*mixed, normed, w_out, w_gate, gain)


def assemble_kernel(planes, chunks, plane_ref, *refs):
    ins, out = refs[:-1], refs[-1]
    plane = plane_ref[0]
    size = ins[0].shape[2]
    for mine in range(planes):

        @pl.when(plane == mine)
        def _(mine=mine):
            for source in range(planes):
                a, b = source & 1, source >> 1
                for g in range(chunks):
                    out[:, 0, a, g * size : (g + 1) * size, b * LANES : (b + 1) * LANES] = ins[
                        (source ^ mine) * chunks + g
                    ][:, 0]


def assemble(plane, pieces, planes):
    chunks = len(pieces) // planes
    depth, blocks, size, width = pieces[0].shape
    step = depth // 4
    return pl.pallas_call(
        functools.partial(assemble_kernel, planes, chunks),
        grid=(4, blocks),
        in_specs=[pl.BlockSpec(memory_space=pltpu.SMEM)]
        + [pl.BlockSpec((step, 1, size, width), lambda d, n: (d, n, 0, 0))] * len(pieces),
        out_specs=pl.BlockSpec((step, 1, 2, chunks * size, 2 * width), lambda d, n: (d, n, 0, 0, 0)),
        out_shape=jax.ShapeDtypeStruct((depth, blocks, 2, chunks * size, 2 * width), BF16),
        compiler_params=pltpu.CompilerParams(dimension_semantics=(ARBITRARY, ARBITRARY)),
        name="assemble",
    )(plane, *pieces)


def block_order(array, order, axis):
    split = array.shape[:axis] + (order.shape[0], array.shape[axis] // order.shape[0]) + array.shape[axis + 1 :]
    return jnp.take(array.reshape(split), order, axis=axis).reshape(array.shape)


def local(
    pair,
    pair_mask,
    in_gain,
    w_left,
    w_left_gate,
    w_right,
    w_right_gate,
    w_out_gate,
    out_gain,
    w_out,
):
    gx, gz = lax.axis_size("gx"), lax.axis_size("gz")
    x, y, z = lax.axis_index("gx"), lax.axis_index("gy"), lax.axis_index("gz")
    plane = z.astype(jnp.int32).reshape(1)
    channels, rows, width = pair.shape
    span = width // 2
    blocks = rows // (2 * span)
    size = span // CHUNKS
    tiles = pair.reshape(channels, blocks, 2, span, width)
    masks = pair_mask.astype(F32).reshape(blocks, 2, span, width)

    stack = jnp.stack([w_left_gate, w_left, w_right_gate, w_right, w_out_gate, w_out])
    weights = lax.all_gather(stack, "gz", axis=2, tiled=True)
    gains = lax.all_gather(out_gain, "gz", axis=0, tiled=True)
    row_order, col_order = jnp.asarray(ROW_ORDER)[z], jnp.asarray(COL_ORDER)[z]
    head_order, plane_order = x ^ jnp.arange(gx), z ^ jnp.arange(gz)

    def pair_weight(gate, linear, order):
        halves = [block_order(block_order(w.T, head_order, 0), order, 1) for w in (gate, linear)]
        return jnp.concatenate(halves, axis=0)

    def lanes(vector):
        return jnp.broadcast_to(vector[:, None], (vector.shape[0], LANES))

    left_weight = pair_weight(weights[0], weights[1], row_order)
    right_weight = pair_weight(weights[2], weights[3], col_order)
    gate_weight = block_order(block_order(weights[4].T, plane_order, 0), row_order, 1)
    out_weight = block_order(block_order(weights[5].T, plane_order, 0), head_order, 1)
    left_gain, right_gain = (lanes(block_order(in_gain, order, 0)) for order in (row_order, col_order))
    mix_gain = lanes(block_order(gains, head_order, 0))
    left_mask = lax.dynamic_index_in_dim(masks, z & 1, 1, keepdims=False)
    right_mask = lax.dynamic_index_in_dim(masks, z >> 1, 1, keepdims=False)

    def send(value, pairs):
        return lax.ppermute(value, "gz", pairs)

    def swap(value, axis, bits):
        return lax.ppermute(value, axis, [(i, i ^ bits) for i in range(lax.axis_size(axis))])

    lefts, rights, normeds = [], [], []
    for g in range(CHUNKS):
        own = [tiles[:, :, p, g * size : (g + 1) * size] for p in range(2)]
        down1 = send(own[0], [(3, 2), (2, 1), (1, 0)])
        up1 = send(own[1], [(0, 1), (1, 2), (2, 3)])
        down2 = send(down1, [(2, 1), (1, 0)])
        up2 = send(up1, [(1, 2), (2, 3)])
        up_side = send(own[0], [(0, 1), (1, 2)])
        down_side = send(own[1], [(3, 2), (2, 1)])
        down3 = send(down2, [(1, 0)])
        up3 = send(up2, [(2, 3)])
        down_late = send(down_side, [(2, 1)])
        up_late = send(up_side, [(1, 2)])
        arrays = own + [down1, up1, down2, up2, down3, up_side, down_side, up3, down_late, up_late]
        col_slots = (
            ((0, (0, 1)), (1, (2, 3))),
            ((2, (0, 1)), (3, (2, 3))),
            ((4, (0, 1)), (5, (2, 3))),
            ((6, (0,)), (7, (1,)), (8, (2,)), (9, (3,))),
        )
        row_slots = (
            ((0, (0, 2)), (1, (1, 3))),
            ((2, (0, 2)), (3, (1, 3))),
            ((4, (0,)), (8, (1,)), (7, (2,)), (5, (3,))),
            ((6, (0,)), (10, (1,)), (11, (2,)), (9, (3,))),
        )
        take = slice(g * size, (g + 1) * size)
        right = project(plane, col_slots, arrays, right_mask[:, take], right_weight, right_gain, gx, False)
        right = [right[0]] + [swap(right[m], "gx", m) for m in range(1, gx)]
        rights.append((right, [swap(value, "gy", 1) for value in right]))
        *left, normed = project(plane, row_slots, arrays, left_mask[:, take], left_weight, left_gain, gx, True)
        lefts.append([left[0]] + [swap(left[m], "gx", m) for m in range(1, gx)])
        normeds.append(normed)

    all_rights = [value for core in range(2) for chunk in rights for value in chunk[core]]
    target = x ^ jnp.arange(gx)
    flags = ((target // blocks) ^ y) * blocks + target % blocks
    pieces = []
    for g in range(CHUNKS):
        mixed = product(flags.astype(jnp.int32), lefts[g], all_rights, 2)
        mixed = [mixed[0]] + [swap(mixed[m], "gx", m) for m in range(1, gx)]
        update = finish(mixed, normeds[g], out_weight, gate_weight, mix_gain, gz)
        pieces.append([update[0]] + [swap(update[q], "gz", q) for q in range(1, gz)])
    ordered = [pieces[g][q] for q in range(gz) for g in range(CHUNKS)]
    return assemble(plane, ordered, gz).reshape(pair.shape)


def plain_local(
    pair,
    pair_mask,
    in_gain,
    w_left,
    w_left_gate,
    w_right,
    w_right_gate,
    w_out_gate,
    out_gain,
    w_out,
):
    gathered = lax.all_gather(pair, "gz", axis=0, tiled=True).astype(F32)
    average = jnp.mean(gathered, axis=0)
    centered = gathered - average
    spread = jnp.mean(jnp.square(centered), axis=0)
    normed = (centered * lax.rsqrt(spread + epsilon) * in_gain[:, None, None]).astype(BF16)
    mask_float = pair_mask.astype(F32)[None]

    def project_all(weight):
        return jnp.einsum("cik,ch->hik", normed, weight, preferred_element_type=F32)

    left_rows = (mask_float * jax.nn.sigmoid(project_all(w_left_gate)) * project_all(w_left)).astype(BF16)
    right_rows = (mask_float * jax.nn.sigmoid(project_all(w_right_gate)) * project_all(w_right)).astype(BF16)
    out_gate = jax.nn.sigmoid(jnp.einsum("cij,cd->dij", normed, w_out_gate, preferred_element_type=F32))
    left_group, right_group = (
        lax.all_to_all(left_rows, "gx", split_axis=0, concat_axis=2, tiled=True),
        lax.all_to_all(right_rows, "gx", split_axis=0, concat_axis=2, tiled=True),
    )
    full_product = lax.dot_general(
        left_group,
        lax.all_gather(right_group, "gy", axis=1, tiled=True),
        (((2,), (2,)), ((0,), (0,))),
        preferred_element_type=F32,
    )
    mixed_sum = lax.all_to_all(full_product, "gx", split_axis=2, concat_axis=0, tiled=True)
    channel_count = lax.axis_size("gz") * mixed_sum.shape[0]
    mix_average = lax.psum(jnp.sum(mixed_sum, axis=0), "gz") / channel_count
    mix_centered = mixed_sum - mix_average
    mix_spread = lax.psum(jnp.sum(jnp.square(mix_centered), axis=0), "gz") / channel_count
    local_mix = (mix_centered * lax.rsqrt(mix_spread + epsilon) * out_gain[:, None, None]).astype(BF16)
    normed_mix = lax.all_gather(local_mix, "gz", axis=0, tiled=True)
    projected = jnp.einsum("hij,hd->dij", normed_mix, w_out, preferred_element_type=F32)
    return (out_gate * projected).astype(BF16)


def solution(mesh):
    placed = (
        P("gz", "gy", "gx"),
        P("gy", "gx"),
        P(),
        P(None, "gz"),
        P(None, "gz"),
        P(None, "gz"),
        P(None, "gz"),
        P(None, "gz"),
        P("gz"),
        P(None, "gz"),
    )
    fits = mesh.shape["gx"] == 4 and mesh.shape["gy"] == 2 and mesh.shape["gz"] == 4
    return jax.shard_map(
        local if fits else plain_local,
        mesh=mesh,
        in_specs=placed,
        out_specs=P("gz", "gy", "gx"),
        check_vma=False,
    )
```

```python
import functools

import jax
import jax.numpy as jnp
from jax import lax
from jax.experimental import pallas as pl
from jax.experimental.pallas import tpu as pltpu
from jax.sharding import PartitionSpec as P


epsilon = 1e-05
CHUNKS = 4
ROWS = 16
PITCH = 24
LANES = 128
F32, BF16 = jnp.float32, jnp.bfloat16
ARBITRARY = pltpu.GridDimensionSemantics.ARBITRARY

ROW_ORDER = ((0, 1, 2, 3), (1, 0, 2, 3), (2, 3, 1, 0), (3, 2, 1, 0))
COL_ORDER = ((0, 1, 2, 3), (1, 2, 3, 0), (2, 1, 0, 3), (3, 2, 1, 0))

MESSAGES = {
    "1": ("own", ((3, 2), (2, 1), (1, 0)), ((0, 1), (1, 2), (2, 3))),
    "2": ("1", ((2, 1), (1, 0)), ((1, 2), (2, 3))),
    "3": ("2", ((1, 0),), ((2, 3),)),
    "s": ("side", ((3, 2), (2, 1)), ((0, 1), (1, 2))),
    "r": ("side", ((3, 2),), ((0, 1),)),
    "t": ("side", ((2, 1),), ((1, 2),)),
    "l": ("far", ((2, 1),), ((1, 2),)),
}
EVENTS = (
    (("1", 0),),
    (("s", 0),),
    (("2", 0),),
    (("1", 1),),
    (("l", 0), ("r", 1), ("3", 0)),
    (("2", 1),),
    (("1", 2),),
    (("t", 1), ("r", 2), ("3", 1)),
    (("2", 2),),
    (("1", 3),),
    (("l", 1), ("r", 3), ("3", 2)),
    (("2", 3),),
    (("t", 2),),
    (("l", 2), ("3", 3)),
    (("t", 3),),
    (("l", 3),),
)
TASKS = {
    6: (("right", 0),),
    7: (("left", 0),),
    9: (("right", 1),),
    10: (("pass", 0),),
    12: (("right", 2),),
    13: (("left", 1),),
    14: (("pass", 1),),
    15: (("right", 3), ("left", 2)),
}
TAIL = (
    ("multiply", 0),
    ("multiply", 1),
    ("share", 3),
    ("multiply", 2),
    ("complete", 0),
    ("complete", 1),
    ("multiply", 3),
    ("complete", 2),
    ("complete", 3),
)


def sigmoid(x):
    return 1.0 / (1.0 + jnp.exp(-x))


def norm_channels(x, gain):
    average = jnp.mean(x, axis=0, keepdims=True)
    centered = x - average
    spread = jnp.mean(jnp.square(centered), axis=0, keepdims=True)
    return (centered * lax.rsqrt(spread + epsilon) * gain).astype(BF16)


def dot(a, b, dims=(((1,), (0,)), ((), ()))):
    return lax.dot_general(a, b, dims, preferred_element_type=F32)


def project_kernel(slots, emit, parts, plane_ref, *refs):
    n_in = sum(len(slot) for slot in slots)
    ins = refs[:n_in]
    mask_ref, weight_ref, gain_ref = refs[n_in : n_in + 3]
    outs = refs[n_in + 3 : n_in + 3 + parts + (1 if emit else 0)]
    x_ref, y_ref = refs[-2:]
    plane = plane_ref[0]
    width = ins[0].shape[-1]
    halves = width // LANES
    channels = ins[0].shape[0]
    position = 0
    for slot_index, slot in enumerate(slots):
        base = slot_index * channels
        for planes in slot:
            source = ins[position]
            position += 1
            hit = functools.reduce(jnp.logical_or, [plane == p for p in planes])

            @pl.when(hit)
            def _(source=source, base=base):
                for half in range(halves):
                    block = source[:, 0, :, half * LANES : (half + 1) * LANES].astype(F32)
                    x_ref[half, base : base + channels, 0:ROWS, :] = block

    total = len(slots) * channels
    hidden = weight_ref.shape[0] // 2
    x_flat = x_ref.reshape(halves, total * PITCH, LANES)
    y_flat = y_ref.reshape(halves, hidden * PITCH, LANES)
    gain = gain_ref[...]

    def step(row, carry):
        normed = [
            norm_channels(x_flat[half, pl.ds(row, total, stride=PITCH), :], gain) for half in range(halves)
        ]
        if emit:
            upper = (plane >> 1) == 1
            chosen = jnp.where(upper, normed[1].astype(F32), normed[0].astype(F32))
            outs[parts][0, row] = chosen.astype(BF16)
        both = dot(weight_ref[...], jnp.concatenate(normed, axis=1))
        mask = mask_ref[0, pl.ds(row, 1), :]
        value = mask * sigmoid(both[:hidden]) * both[hidden:]
        for half in range(halves):
            y_flat[half, pl.ds(row, hidden, stride=PITCH), :] = value[:, half * LANES : (half + 1) * LANES]
        return carry

    lax.fori_loop(0, ROWS, step, 0, unroll=8)
    part = hidden // parts
    for m in range(parts):
        for half in range(halves):
            block = y_ref[half, m * part : (m + 1) * part, 0:ROWS, :]
            outs[m][:, 0, :, half * LANES : (half + 1) * LANES] = block.astype(BF16)


def project(plane, slots, arrays, mask, weight, gain, parts, emit):
    channels, blocks, size, width = arrays[0].shape
    hidden = weight.shape[0] // 2
    total = len(slots) * channels
    planes = tuple(tuple(p for _, p in slot) for slot in slots)
    ins = [arrays[index] for slot in slots for index, _ in slot]
    block = pl.BlockSpec((channels, 1, ROWS, width), lambda n, t: (0, n, t, 0))
    whole = lambda n, t: (0, 0)
    out_specs = [pl.BlockSpec((hidden // parts, 1, ROWS, width), lambda n, t: (0, n, t, 0))] * parts
    out_shape = [jax.ShapeDtypeStruct((hidden // parts, blocks, size, width), BF16)] * parts
    if emit:
        out_specs = out_specs + [pl.BlockSpec((1, ROWS, total, LANES), lambda n, t: (n, t, 0, 0))]
        out_shape = out_shape + [jax.ShapeDtypeStruct((blocks, size, total, LANES), BF16)]
    pixels = blocks * size * width
    return pl.pallas_call(
        functools.partial(project_kernel, planes, emit, parts),
        grid=(blocks, size // ROWS),
        in_specs=[pl.BlockSpec(memory_space=pltpu.SMEM)]
        + [block] * len(ins)
        + [
            pl.BlockSpec((1, ROWS, width), lambda n, t: (n, t, 0)),
            pl.BlockSpec(weight.shape, whole),
            pl.BlockSpec(gain.shape, whole),
        ],
        out_specs=out_specs,
        out_shape=out_shape,
        scratch_shapes=[
            pltpu.VMEM((width // LANES, total, PITCH, LANES), F32),
            pltpu.VMEM((width // LANES, hidden, PITCH, LANES), F32),
        ],
        compiler_params=pltpu.CompilerParams(dimension_semantics=(ARBITRARY, ARBITRARY)),
        cost_estimate=pl.CostEstimate(
            flops=16 * pixels * total * hidden, bytes_accessed=2 * pixels * (total * 3 + hidden), transcendentals=0
        ),
        name="project",
    )(plane, *ins, mask, weight, gain)


def product_kernel(parts, chunks, left_chunks, target_ref, *refs):
    lefts = refs[: left_chunks * parts]
    rights = refs[left_chunks * parts : (left_chunks + 2 * chunks) * parts]
    outs = refs[(left_chunks + 2 * chunks) * parts :]
    heads, blocks, size, _ = lefts[0].shape
    cores = 2
    for head in range(heads):
        rows = [
            jnp.concatenate([lefts[c * parts + m][head, n] for m in range(parts)], axis=1)
            for n in range(blocks)
            for c in range(left_chunks)
        ]
        left = jnp.concatenate(rows, axis=0)
        rows = [
            jnp.concatenate([rights[(core * chunks + g) * parts + m][head, n] for m in range(parts)], axis=1)
            for core in range(cores)
            for n in range(blocks)
            for g in range(chunks)
        ]
        right = jnp.concatenate(rows, axis=0)
        mixed = dot(left, right, (((1,), (1,)), ((), ())))
        span = chunks * size
        pieces = [mixed[:, p * span : (p + 1) * span] for p in range(cores * blocks)]
        for m in range(parts):
            pick = target_ref[m]
            value = pieces[0]
            for p in range(1, len(pieces)):
                value = jnp.where(pick == p, pieces[p], value)
            outs[m][head] = value.astype(BF16).reshape(blocks, left_chunks * size, span)


def product(target, lefts, rights, parts, heads):
    hidden, blocks, size, width = lefts[0].shape
    cores = 2
    chunks, left_chunks = len(rights) // (cores * parts), len(lefts) // parts
    span = chunks * size
    left_block = pl.BlockSpec((heads, blocks, size, width), lambda h: (h, 0, 0, 0))
    rows = left_chunks * blocks * size
    return pl.pallas_call(
        functools.partial(product_kernel, parts, chunks, left_chunks),
        grid=(hidden // heads,),
        in_specs=[pl.BlockSpec(memory_space=pltpu.SMEM)] + [left_block] * (len(lefts) + len(rights)),
        out_specs=[pl.BlockSpec((heads, blocks, left_chunks * size, span), lambda h: (h, 0, 0, 0))] * parts,
        out_shape=[jax.ShapeDtypeStruct((hidden, blocks, left_chunks * size, span), BF16)] * parts,
        compiler_params=pltpu.CompilerParams(dimension_semantics=(ARBITRARY,)),
        cost_estimate=pl.CostEstimate(
            flops=2 * hidden * rows * (cores * blocks * span) * width * parts,
            bytes_accessed=2 * hidden * width * parts * (rows + cores * blocks * span),
            transcendentals=0,
        ),
        name="product",
    )(target, *lefts, *rights)


def finish_kernel(parts, *refs):
    mixed = refs[:parts]
    normed_ref, out_ref, gate_ref, gain_ref = refs[parts : parts + 4]
    outs = refs[parts + 4 : -2]
    x_ref, y_ref = refs[-2:]
    part = mixed[0].shape[0]
    for m in range(parts):
        x_ref[m * part : (m + 1) * part, 0:ROWS, :] = mixed[m][:, 0].astype(F32)
    total = parts * part
    x_flat = x_ref.reshape(total * PITCH, LANES)
    y_flat = y_ref.reshape(out_ref.shape[0] * PITCH, LANES)
    gain = gain_ref[...]
    together = 2

    def step(pair, carry):
        base = pair * together
        normed = [
            norm_channels(x_flat[pl.ds(base + r, total, stride=PITCH), :], gain) for r in range(together)
        ]
        gates = dot(gate_ref[...], jnp.concatenate([normed_ref[0, base + r] for r in range(together)], axis=1))
        value = sigmoid(gates) * dot(out_ref[...], jnp.concatenate(normed, axis=1))
        for r in range(together):
            y_flat[pl.ds(base + r, value.shape[0], stride=PITCH), :] = value[:, r * LANES : (r + 1) * LANES]
        return carry

    lax.fori_loop(0, ROWS // together, step, 0, unroll=4)
    part = out_ref.shape[0] // len(outs)
    for q, out in enumerate(outs):
        block = y_ref[q * part : (q + 1) * part, 0:ROWS, :]
        out[:, 0] = block.astype(BF16)


def finish(mixed, normed, offset, w_out, w_gate, gain, planes):
    part, width = mixed[0].shape[0], mixed[0].shape[-1]
    blocks, size = normed.shape[:2]
    first = offset // ROWS
    depth = w_out.shape[0]
    total = part * len(mixed)
    whole = lambda n, t: (0, 0)
    pixels = blocks * size * width
    return pl.pallas_call(
        functools.partial(finish_kernel, len(mixed)),
        grid=(blocks, size // ROWS),
        in_specs=[pl.BlockSpec((part, 1, ROWS, width), lambda n, t: (0, n, t + first, 0))] * len(mixed)
        + [
            pl.BlockSpec((1, ROWS, normed.shape[2], width), lambda n, t: (n, t, 0, 0)),
            pl.BlockSpec(w_out.shape, whole),
            pl.BlockSpec(w_gate.shape, whole),
            pl.BlockSpec(gain.shape, whole),
        ],
        out_specs=[pl.BlockSpec((depth // planes, 1, ROWS, width), lambda n, t: (0, n, t, 0))] * planes,
        out_shape=[jax.ShapeDtypeStruct((depth // planes, blocks, size, width), BF16)] * planes,
        scratch_shapes=[pltpu.VMEM((total, PITCH, width), F32), pltpu.VMEM((depth, PITCH, width), F32)],
        compiler_params=pltpu.CompilerParams(dimension_semantics=(ARBITRARY, ARBITRARY)),
        cost_estimate=pl.CostEstimate(
            flops=16 * pixels * total * depth, bytes_accessed=2 * pixels * total * 3, transcendentals=0
        ),
        name="finish",
    )(*mixed, normed, w_out, w_gate, gain)


def assemble_kernel(planes, chunks, plane_ref, *refs):
    ins, out = refs[:-1], refs[-1]
    plane = plane_ref[0]
    size = ins[0].shape[2]
    for mine in range(planes):

        @pl.when(plane == mine)
        def _(mine=mine):
            for source in range(planes):
                a, b = source & 1, source >> 1
                for g in range(chunks):
                    out[:, 0, a, g * size : (g + 1) * size, b * LANES : (b + 1) * LANES] = ins[
                        (source ^ mine) * chunks + g
                    ][:, 0]


def assemble(plane, pieces, planes):
    chunks = len(pieces) // planes
    depth, blocks, size, width = pieces[0].shape
    step = depth // 4
    return pl.pallas_call(
        functools.partial(assemble_kernel, planes, chunks),
        grid=(4, blocks),
        in_specs=[pl.BlockSpec(memory_space=pltpu.SMEM)]
        + [pl.BlockSpec((step, 1, size, width), lambda d, n: (d, n, 0, 0))] * len(pieces),
        out_specs=pl.BlockSpec((step, 1, 2, chunks * size, 2 * width), lambda d, n: (d, n, 0, 0, 0)),
        out_shape=jax.ShapeDtypeStruct((depth, blocks, 2, chunks * size, 2 * width), BF16),
        compiler_params=pltpu.CompilerParams(dimension_semantics=(ARBITRARY, ARBITRARY)),
        name="assemble",
    )(plane, *pieces)


def block_order(array, order, axis):
    split = array.shape[:axis] + (order.shape[0], array.shape[axis] // order.shape[0]) + array.shape[axis + 1 :]
    return jnp.take(array.reshape(split), order, axis=axis).reshape(array.shape)


def local(
    pair,
    pair_mask,
    in_gain,
    w_left,
    w_left_gate,
    w_right,
    w_right_gate,
    w_out_gate,
    out_gain,
    w_out,
):
    gx, gz = lax.axis_size("gx"), lax.axis_size("gz")
    x, y, z = lax.axis_index("gx"), lax.axis_index("gy"), lax.axis_index("gz")
    plane = z.astype(jnp.int32).reshape(1)
    channels, rows, width = pair.shape
    span = width // 2
    blocks = rows // (2 * span)
    size = span // CHUNKS
    tiles = pair.reshape(channels, blocks, 2, span, width)
    masks = pair_mask.astype(F32).reshape(blocks, 2, span, width)

    shared = [w_left_gate, w_left, w_right_gate, w_right, w_out_gate, w_out, out_gain[None]]
    shared = lax.all_gather(jnp.concatenate([w.astype(F32) for w in shared], axis=0), "gz", axis=1, tiled=True)
    tiles, shared = lax.optimization_barrier((tiles, shared))
    weights = [shared[i * channels * gz : (i + 1) * channels * gz].astype(BF16) for i in range(6)]
    gains = shared[-1]
    row_order, col_order = jnp.asarray(ROW_ORDER)[z], jnp.asarray(COL_ORDER)[z]
    head_order, plane_order = x ^ jnp.arange(gx), z ^ jnp.arange(gz)

    def pair_weight(gate, linear, order):
        halves = [block_order(block_order(w.T, head_order, 0), order, 1) for w in (gate, linear)]
        return jnp.concatenate(halves, axis=0)

    def lanes(vector):
        return jnp.broadcast_to(vector[:, None], (vector.shape[0], LANES))

    left_weight = pair_weight(weights[0], weights[1], row_order)
    right_weight = pair_weight(weights[2], weights[3], col_order)
    gate_weight = block_order(block_order(weights[4].T, plane_order, 0), row_order, 1)
    out_weight = block_order(block_order(weights[5].T, plane_order, 0), head_order, 1)
    left_gain, right_gain = (lanes(block_order(in_gain, order, 0)) for order in (row_order, col_order))
    mix_gain = lanes(block_order(gains, head_order, 0))
    left_mask = lax.dynamic_index_in_dim(masks, z & 1, 1, keepdims=False)
    right_mask = lax.dynamic_index_in_dim(masks, z >> 1, 1, keepdims=False)

    values = {}

    def sync(*keys):
        keys = list(dict.fromkeys(keys))
        values.update(zip(keys, lax.optimization_barrier(tuple(values[key] for key in keys))))

    def start(kind, g):
        operand, down, up = MESSAGES[kind]
        sources = (1, 0) if operand == "side" else (0, 1)
        if operand == "far":
            operand = "s" if ("s", g, 0) in values else "r"
        for way, pairs in enumerate((down, up)):
            source = ("own", g, sources[way]) if operand in ("own", "side") else (operand, g, way)
            values[kind, g, way] = lax.ppermute(values[source], "gz", pairs)

    def operands(kind, g):
        operand = MESSAGES[kind][0]
        if operand == "far":
            operand = "s" if ("s", g, 0) in values else "r"
        return [("own" if operand == "side" else operand, g, way) for way in range(2)]

    def swap(value, axis, bits):
        return lax.ppermute(value, axis, [(i, i ^ bits) for i in range(lax.axis_size(axis))])

    def share(name, g):
        for m in range(1, gx):
            values[name, g, m] = swap(values[name, g, m], "gx", m)

    def pass_on(g):
        for m in range(gx):
            values["other", g, m] = swap(values["right", g, m], "gy", 1)

    def sides(g):
        far, near = ("s", "s") if ("s", g, 0) in values else ("r", "t")
        return [values[far, g, way] for way in range(2)], [values.get((near, g, way)) for way in range(2)]

    def project_right(g):
        (far_down, far_up), _ = sides(g)
        arrays = [values[key, g, way] for key in ("own", "1", "2", "3") for way in range(2)] + [far_down, far_up]
        slots = (
            ((0, (0, 1)), (1, (2, 3))),
            ((2, (0, 1)), (3, (2, 3))),
            ((4, (0, 1)), (5, (2, 3))),
            ((6, (0,)), (9, (1,)), (8, (2,)), (7, (3,))),
        )
        mask = right_mask[:, g * size : (g + 1) * size]
        outs = project(plane, slots, arrays, mask, right_weight, right_gain, gx, False)
        values.update({("right", g, m): outs[m] for m in range(gx)})

    def project_left(g):
        _, (near_down, near_up) = sides(g)
        arrays = [values[key, g, way] for key in ("own", "1", "2", "3", "l") for way in range(2)] + [near_down, near_up]
        slots = (
            ((0, (0, 2)), (1, (1, 3))),
            ((2, (0, 2)), (3, (1, 3))),
            ((4, (0,)), (10, (1,)), (11, (2,)), (5, (3,))),
            ((6, (0,)), (8, (1,)), (9, (2,)), (7, (3,))),
        )
        mask = left_mask[:, g * size : (g + 1) * size]
        outs = project(plane, slots, arrays, mask, left_weight, left_gain, gx, True)
        values.update({("left", g, m): outs[m] for m in range(gx)})
        values["normed", g] = outs[gx]

    target = (((x // blocks) ^ y) * blocks + x % blocks) ^ jnp.arange(gx)
    target = target.astype(jnp.int32)

    def multiply(g):
        rights = [values[key, c, m] for key in ("right", "other") for c in range(CHUNKS) for m in range(gx)]
        outs = product(target, [values["left", g, m] for m in range(gx)], rights, gx, 2)
        values.update({("mixed", g, m): outs[m] for m in range(gx)})

    def complete(g):
        mixed = [values["mixed", g, m] for m in range(gx)]
        outs = finish(mixed, values["normed", g], 0, out_weight, gate_weight, mix_gain, gz)
        values.update({("out", g, q): outs[q] for q in range(gz)})
        for q in range(1, gz):
            values["out", g, q] = swap(outs[q], "gz", q)

    for g in range(CHUNKS):
        for p in range(2):
            values["own", g, p] = tiles[:, :, p, g * size : (g + 1) * size]

    waits = []
    for e, messages in enumerate(EVENTS):
        keys = [(kind, g, way) for kind, g in EVENTS[e - 2] for way in range(2)] if e >= 2 else []
        keys += [key for kind, g in messages for key in operands(kind, g)]
        sync(*keys, *waits)
        waits = []
        for kind, g in messages:
            start(kind, g)
        for name, g in TASKS.get(e, ()):
            if name == "pass":
                pass_on(g)
            else:
                (project_right if name == "right" else project_left)(g)
                share(name, g)
                waits.append((name, g, 0))
        for name, g in TASKS.get(e + 1, ()):
            if name == "pass":
                waits += [("right", g, m) for m in range(gx)]
        for name, g in TASKS.get(e - 1, ()):
            if name == "pass":
                waits += [("other", g, m) for m in range(gx)]

    last = CHUNKS - 1
    sync(*waits, *[(kind, g, way) for event in EVENTS[-2:] for kind, g in event for way in range(2)])
    project_left(last)
    sync(("left", last, 0), *[("right", last - 1, m) for m in range(gx)])
    pass_on(last - 1)
    sync(*[("right", g, m) for g in (last - 1, last) for m in range(gx)])
    pass_on(last)
    previous = None
    for step, g in TAIL:
        needs = {"multiply": ["left"], "complete": ["mixed"], "share": ["left"]}[step]
        keys = [(name, g, m) for name in needs for m in range(gx)]
        sync(*keys, *([previous] if previous else []))
        if step == "multiply":
            multiply(g)
            previous = ("mixed", g, 0)
            share("mixed", g)
        elif step == "share":
            share("left", g)
        else:
            complete(g)
            previous = ("out", g, 0)
    ordered = [values["out", g, q] for q in range(gz) for g in range(CHUNKS)]
    return assemble(plane, ordered, gz).reshape(pair.shape)


def plain_local(
    pair,
    pair_mask,
    in_gain,
    w_left,
    w_left_gate,
    w_right,
    w_right_gate,
    w_out_gate,
    out_gain,
    w_out,
):
    gathered = lax.all_gather(pair, "gz", axis=0, tiled=True).astype(F32)
    average = jnp.mean(gathered, axis=0)
    centered = gathered - average
    spread = jnp.mean(jnp.square(centered), axis=0)
    normed = (centered * lax.rsqrt(spread + epsilon) * in_gain[:, None, None]).astype(BF16)
    mask_float = pair_mask.astype(F32)[None]

    def project_all(weight):
        return jnp.einsum("cik,ch->hik", normed, weight, preferred_element_type=F32)

    left_rows = (mask_float * jax.nn.sigmoid(project_all(w_left_gate)) * project_all(w_left)).astype(BF16)
    right_rows = (mask_float * jax.nn.sigmoid(project_all(w_right_gate)) * project_all(w_right)).astype(BF16)
    out_gate = jax.nn.sigmoid(jnp.einsum("cij,cd->dij", normed, w_out_gate, preferred_element_type=F32))
    left_group, right_group = (
        lax.all_to_all(left_rows, "gx", split_axis=0, concat_axis=2, tiled=True),
        lax.all_to_all(right_rows, "gx", split_axis=0, concat_axis=2, tiled=True),
    )
    full_product = lax.dot_general(
        left_group,
        lax.all_gather(right_group, "gy", axis=1, tiled=True),
        (((2,), (2,)), ((0,), (0,))),
        preferred_element_type=F32,
    )
    mixed_sum = lax.all_to_all(full_product, "gx", split_axis=2, concat_axis=0, tiled=True)
    channel_count = lax.axis_size("gz") * mixed_sum.shape[0]
    mix_average = lax.psum(jnp.sum(mixed_sum, axis=0), "gz") / channel_count
    mix_centered = mixed_sum - mix_average
    mix_spread = lax.psum(jnp.sum(jnp.square(mix_centered), axis=0), "gz") / channel_count
    local_mix = (mix_centered * lax.rsqrt(mix_spread + epsilon) * out_gain[:, None, None]).astype(BF16)
    normed_mix = lax.all_gather(local_mix, "gz", axis=0, tiled=True)
    projected = jnp.einsum("hij,hd->dij", normed_mix, w_out, preferred_element_type=F32)
    return (out_gate * projected).astype(BF16)


def solution(mesh):
    placed = (
        P("gz", "gy", "gx"),
        P("gy", "gx"),
        P(),
        P(None, "gz"),
        P(None, "gz"),
        P(None, "gz"),
        P(None, "gz"),
        P(None, "gz"),
        P("gz"),
        P(None, "gz"),
    )
    fits = mesh.shape["gx"] == 4 and mesh.shape["gy"] == 2 and mesh.shape["gz"] == 4

    def step(*args):
        return local(*args) if fits else plain_local(*args)

    step = jax.shard_map(step, mesh=mesh, in_specs=placed, out_specs=P("gz", "gy", "gx"), check_vma=False)
    return step
```

```python
import functools

import jax
import jax.numpy as jnp
from jax import lax
from jax.experimental import pallas as pl
from jax.experimental.pallas import tpu as pltpu
from jax.sharding import PartitionSpec as P


epsilon = 1e-05
CHUNKS = 4
ROWS = 16
PITCH = 24
LANES = 128
F32, BF16 = jnp.float32, jnp.bfloat16
ARBITRARY = pltpu.GridDimensionSemantics.ARBITRARY

ROW_ORDER = ((0, 1, 2, 3), (1, 0, 2, 3), (2, 3, 1, 0), (3, 2, 1, 0))
COL_ORDER = ((0, 1, 2, 3), (1, 2, 3, 0), (2, 1, 0, 3), (3, 2, 1, 0))

HOPS = {
    "1d": ((3, 2), (2, 1), (1, 0)),
    "1u": ((0, 1), (1, 2), (2, 3)),
    "2d": ((2, 1), (1, 0)),
    "2u": ((1, 2), (2, 3)),
    "x": ((0, 1), (1, 0), (2, 3), (3, 2)),
    "t": ((0, 0), (1, 2), (2, 1), (3, 3)),
    "l": ((0, 0), (1, 2), (2, 1), (3, 3)),
}
EVENTS = (
    (("1", 0),),
    (("x", None, 0), ("t", 0)),
    (("2", 0),),
    (("1", 1),),
    (("l", 0), ("x", 0, 1)),
    (("2", 1),),
    (("1", 2),),
    (("t", 1), ("x", 1, 2)),
    (("2", 2),),
    (("1", 3),),
    (("l", 1), ("x", 2, 3)),
    (("2", 3),),
    (("t", 2),),
    (("l", 2), ("x", 3, None)),
    (("t", 3),),
    (("l", 3),),
)
TASKS = {
    6: (("right", 0),),
    7: (("left", 0),),
    9: (("right", 1),),
    10: (("pass", 0),),
    12: (("right", 2),),
    13: (("left", 1),),
    14: (("pass", 1),),
    15: (("right", 3), ("left", 2)),
}
TAIL = (
    ("multiply", (0, 1)),
    ("multiply", (2,)),
    ("complete", 0),
    ("share", 3),
    ("complete", 1),
    ("complete", 2),
    ("multiply", (3,)),
    ("complete", 3),
)


def sigmoid(x):
    return 1.0 / (1.0 + jnp.exp(-x))


def norm_channels(x, gain):
    average = jnp.mean(x, axis=0, keepdims=True)
    centered = x - average
    spread = jnp.mean(jnp.square(centered), axis=0, keepdims=True)
    return (centered * lax.rsqrt(spread + epsilon) * gain).astype(BF16)


def dot(a, b, dims=(((1,), (0,)), ((), ()))):
    return lax.dot_general(a, b, dims, preferred_element_type=F32)


def project_kernel(slots, emit, parts, plane_ref, *refs):
    n_in = sum(len(slot) for slot in slots)
    ins = refs[:n_in]
    mask_ref, weight_ref, gain_ref = refs[n_in : n_in + 3]
    outs = refs[n_in + 3 : n_in + 3 + parts + (1 if emit else 0)]
    x_ref, y_ref = refs[-2:]
    plane = plane_ref[0]
    width = ins[0].shape[-1]
    halves = width // LANES
    channels = ins[0].shape[0]
    position = 0
    for slot_index, slot in enumerate(slots):
        base = slot_index * channels
        for planes in slot:
            source = ins[position]
            position += 1
            hit = functools.reduce(jnp.logical_or, [plane == p for p in planes])

            @pl.when(hit)
            def _(source=source, base=base):
                for half in range(halves):
                    block = source[:, 0, :, half * LANES : (half + 1) * LANES].astype(F32)
                    x_ref[half, base : base + channels, 0:ROWS, :] = block

    total = len(slots) * channels
    hidden = weight_ref.shape[0] // 2
    x_flat = x_ref.reshape(halves, total * PITCH, LANES)
    y_flat = y_ref.reshape(halves, hidden * PITCH, LANES)
    gain = gain_ref[...]

    def step(row, carry):
        normed = [
            norm_channels(x_flat[half, pl.ds(row, total, stride=PITCH), :], gain) for half in range(halves)
        ]
        if emit:
            upper = (plane >> 1) == 1
            chosen = jnp.where(upper, normed[1].astype(F32), normed[0].astype(F32))
            outs[parts][0, row] = chosen.astype(BF16)
        both = dot(weight_ref[...], jnp.concatenate(normed, axis=1))
        mask = mask_ref[0, pl.ds(row, 1), :]
        value = mask * sigmoid(both[:hidden]) * both[hidden:]
        for half in range(halves):
            y_flat[half, pl.ds(row, hidden, stride=PITCH), :] = value[:, half * LANES : (half + 1) * LANES]
        return carry

    lax.fori_loop(0, ROWS, step, 0, unroll=8)
    part = hidden // parts
    for m in range(parts):
        for half in range(halves):
            block = y_ref[half, m * part : (m + 1) * part, 0:ROWS, :]
            outs[m][:, 0, :, half * LANES : (half + 1) * LANES] = block.astype(BF16)


def project(plane, slots, arrays, mask, weight, gain, parts, emit):
    channels, blocks, size, width = arrays[0].shape
    hidden = weight.shape[0] // 2
    total = len(slots) * channels
    planes = tuple(tuple(p for _, p in slot) for slot in slots)
    ins = [arrays[index] for slot in slots for index, _ in slot]
    block = pl.BlockSpec((channels, 1, ROWS, width), lambda n, t: (0, n, t, 0))
    whole = lambda n, t: (0, 0)
    out_specs = [pl.BlockSpec((hidden // parts, 1, ROWS, width), lambda n, t: (0, n, t, 0))] * parts
    out_shape = [jax.ShapeDtypeStruct((hidden // parts, blocks, size, width), BF16)] * parts
    if emit:
        out_specs = out_specs + [pl.BlockSpec((1, ROWS, total, LANES), lambda n, t: (n, t, 0, 0))]
        out_shape = out_shape + [jax.ShapeDtypeStruct((blocks, size, total, LANES), BF16)]
    pixels = blocks * size * width
    return pl.pallas_call(
        functools.partial(project_kernel, planes, emit, parts),
        grid=(blocks, size // ROWS),
        in_specs=[pl.BlockSpec(memory_space=pltpu.SMEM)]
        + [block] * len(ins)
        + [
            pl.BlockSpec((1, ROWS, width), lambda n, t: (n, t, 0)),
            pl.BlockSpec(weight.shape, whole),
            pl.BlockSpec(gain.shape, whole),
        ],
        out_specs=out_specs,
        out_shape=out_shape,
        scratch_shapes=[
            pltpu.VMEM((width // LANES, total, PITCH, LANES), F32),
            pltpu.VMEM((width // LANES, hidden, PITCH, LANES), F32),
        ],
        compiler_params=pltpu.CompilerParams(dimension_semantics=(ARBITRARY, ARBITRARY)),
        cost_estimate=pl.CostEstimate(
            flops=16 * pixels * total * hidden, bytes_accessed=2 * pixels * (total * 3 + hidden), transcendentals=0
        ),
        name="project",
    )(plane, *ins, mask, weight, gain)


def product_kernel(parts, chunks, left_chunks, target_ref, *refs):
    lefts = refs[: left_chunks * parts]
    rights = refs[left_chunks * parts : (left_chunks + 2 * chunks) * parts]
    outs = refs[(left_chunks + 2 * chunks) * parts :]
    heads, blocks, size, _ = lefts[0].shape
    cores = 2
    for head in range(heads):
        rows = [
            jnp.concatenate([lefts[c * parts + m][head, n] for m in range(parts)], axis=1)
            for c in range(left_chunks)
            for n in range(blocks)
        ]
        left = jnp.concatenate(rows, axis=0)
        rows = [
            jnp.concatenate([rights[(core * chunks + g) * parts + m][head, n] for m in range(parts)], axis=1)
            for core in range(cores)
            for n in range(blocks)
            for g in range(chunks)
        ]
        right = jnp.concatenate(rows, axis=0)
        mixed = dot(left, right, (((1,), (1,)), ((), ())))
        span = chunks * size
        pieces = [mixed[:, p * span : (p + 1) * span] for p in range(cores * blocks)]
        for m in range(parts):
            pick = target_ref[m]
            value = pieces[0]
            for p in range(1, len(pieces)):
                value = jnp.where(pick == p, pieces[p], value)
            value = value.astype(BF16)
            for c in range(left_chunks):
                rows = blocks * size
                outs[c * parts + m][head] = value[c * rows : (c + 1) * rows].reshape(blocks, size, span)


def product(target, lefts, rights, parts, heads):
    hidden, blocks, size, width = lefts[0].shape
    cores = 2
    chunks, left_chunks = len(rights) // (cores * parts), len(lefts) // parts
    span = chunks * size
    left_block = pl.BlockSpec((heads, blocks, size, width), lambda h: (h, 0, 0, 0))
    rows = left_chunks * blocks * size
    return pl.pallas_call(
        functools.partial(product_kernel, parts, chunks, left_chunks),
        grid=(hidden // heads,),
        in_specs=[pl.BlockSpec(memory_space=pltpu.SMEM)] + [left_block] * (len(lefts) + len(rights)),
        out_specs=[pl.BlockSpec((heads, blocks, size, span), lambda h: (h, 0, 0, 0))] * len(lefts),
        out_shape=[jax.ShapeDtypeStruct((hidden, blocks, size, span), BF16)] * len(lefts),
        compiler_params=pltpu.CompilerParams(dimension_semantics=(ARBITRARY,)),
        cost_estimate=pl.CostEstimate(
            flops=2 * hidden * rows * (cores * blocks * span) * width * parts,
            bytes_accessed=2 * hidden * width * parts * (rows + cores * blocks * span),
            transcendentals=0,
        ),
        name="product",
    )(target, *lefts, *rights)


def finish_kernel(parts, *refs):
    mixed = refs[:parts]
    normed_ref, out_ref, gate_ref, gain_ref = refs[parts : parts + 4]
    outs = refs[parts + 4 : -2]
    x_ref, y_ref = refs[-2:]
    part = mixed[0].shape[0]
    for m in range(parts):
        x_ref[m * part : (m + 1) * part, 0:ROWS, :] = mixed[m][:, 0].astype(F32)
    total = parts * part
    x_flat = x_ref.reshape(total * PITCH, LANES)
    y_flat = y_ref.reshape(out_ref.shape[0] * PITCH, LANES)
    gain = gain_ref[...]
    together = 2

    def step(pair, carry):
        base = pair * together
        normed = [
            norm_channels(x_flat[pl.ds(base + r, total, stride=PITCH), :], gain) for r in range(together)
        ]
        gates = dot(gate_ref[...], jnp.concatenate([normed_ref[0, base + r] for r in range(together)], axis=1))
        value = sigmoid(gates) * dot(out_ref[...], jnp.concatenate(normed, axis=1))
        for r in range(together):
            y_flat[pl.ds(base + r, value.shape[0], stride=PITCH), :] = value[:, r * LANES : (r + 1) * LANES]
        return carry

    lax.fori_loop(0, ROWS // together, step, 0, unroll=4)
    part = out_ref.shape[0] // len(outs)
    for q, out in enumerate(outs):
        block = y_ref[q * part : (q + 1) * part, 0:ROWS, :]
        out[:, 0] = block.astype(BF16)


def finish(mixed, normed, offset, w_out, w_gate, gain, planes):
    part, width = mixed[0].shape[0], mixed[0].shape[-1]
    blocks, size = normed.shape[:2]
    first = offset // ROWS
    depth = w_out.shape[0]
    total = part * len(mixed)
    whole = lambda n, t: (0, 0)
    pixels = blocks * size * width
    return pl.pallas_call(
        functools.partial(finish_kernel, len(mixed)),
        grid=(blocks, size // ROWS),
        in_specs=[pl.BlockSpec((part, 1, ROWS, width), lambda n, t: (0, n, t + first, 0))] * len(mixed)
        + [
            pl.BlockSpec((1, ROWS, normed.shape[2], width), lambda n, t: (n, t, 0, 0)),
            pl.BlockSpec(w_out.shape, whole),
            pl.BlockSpec(w_gate.shape, whole),
            pl.BlockSpec(gain.shape, whole),
        ],
        out_specs=[pl.BlockSpec((depth // planes, 1, ROWS, width), lambda n, t: (0, n, t, 0))] * planes,
        out_shape=[jax.ShapeDtypeStruct((depth // planes, blocks, size, width), BF16)] * planes,
        scratch_shapes=[pltpu.VMEM((total, PITCH, width), F32), pltpu.VMEM((depth, PITCH, width), F32)],
        compiler_params=pltpu.CompilerParams(dimension_semantics=(ARBITRARY, ARBITRARY)),
        cost_estimate=pl.CostEstimate(
            flops=16 * pixels * total * depth, bytes_accessed=2 * pixels * total * 3, transcendentals=0
        ),
        name="finish",
    )(*mixed, normed, w_out, w_gate, gain)


def assemble_kernel(planes, chunks, plane_ref, *refs):
    ins, out = refs[: planes * chunks], refs[-1]
    plane = plane_ref[0]
    size = ins[0].shape[2]
    for mine in range(planes):

        @pl.when(plane == mine)
        def _(mine=mine):
            for source in range(planes):
                a, b = source & 1, source >> 1
                for g in range(chunks):
                    out[:, 0, a, g * size : (g + 1) * size, b * LANES : (b + 1) * LANES] = ins[
                        (source ^ mine) * chunks + g
                    ][:, 0]


def assemble(plane, pieces, planes, position, count, base=None):
    chunks = len(pieces) // planes
    depth, blocks, size, width = pieces[0].shape
    step = depth // 4
    out_block = (step, 1, 2, chunks * size, 2 * width)
    return pl.pallas_call(
        functools.partial(assemble_kernel, planes, chunks),
        grid=(4, blocks),
        in_specs=[pl.BlockSpec(memory_space=pltpu.SMEM)]
        + [pl.BlockSpec((step, 1, size, width), lambda d, n: (d, n, 0, 0))] * len(pieces)
        + ([] if base is None else [pl.BlockSpec(memory_space=pl.ANY)]),
        out_specs=pl.BlockSpec(out_block, lambda d, n: (d, n, 0, position // chunks, 0)),
        out_shape=jax.ShapeDtypeStruct((depth, blocks, 2, count * size, 2 * width), BF16),
        input_output_aliases={} if base is None else {1 + len(pieces): 0},
        compiler_params=pltpu.CompilerParams(dimension_semantics=(ARBITRARY, ARBITRARY)),
        cost_estimate=pl.CostEstimate(
            flops=4 * depth * blocks * size * width * len(pieces),
            bytes_accessed=4 * depth * blocks * size * width * len(pieces),
            transcendentals=0,
        ),
        name="assemble",
    )(plane, *pieces, *(() if base is None else (base,)))


def block_order(array, order, axis):
    split = array.shape[:axis] + (order.shape[0], array.shape[axis] // order.shape[0]) + array.shape[axis + 1 :]
    return jnp.take(array.reshape(split), order, axis=axis).reshape(array.shape)


def local(
    pair,
    pair_mask,
    in_gain,
    w_left,
    w_left_gate,
    w_right,
    w_right_gate,
    w_out_gate,
    out_gain,
    w_out,
):
    gx, gz = lax.axis_size("gx"), lax.axis_size("gz")
    x, y, z = lax.axis_index("gx"), lax.axis_index("gy"), lax.axis_index("gz")
    plane = z.astype(jnp.int32).reshape(1)
    channels, rows, width = pair.shape
    span = width // 2
    blocks = rows // (2 * span)
    size = span // CHUNKS
    tiles = pair.reshape(channels, blocks, 2, span, width)
    masks = pair_mask.astype(F32).reshape(blocks, 2, span, width)
    left_mask = lax.dynamic_index_in_dim(masks, z & 1, 1, keepdims=False)
    right_mask = lax.dynamic_index_in_dim(masks, z >> 1, 1, keepdims=False)
    held = (w_left_gate, w_left, w_right_gate, w_right, w_out_gate, w_out, out_gain)

    values = {}

    def sync(*keys):
        keys = list(dict.fromkeys(keys))
        values.update(zip(keys, lax.optimization_barrier(tuple(values[key] for key in keys))))

    def by_plane(*choices):
        value = choices[-1]
        for p, choice in list(enumerate(choices))[-2::-1]:
            value = jnp.where(z == p, choice, value)
        return value

    def sources(message):
        kind, *chunk = message
        if kind == "1":
            return [("own", chunk[0], p) for p in range(2)]
        if kind == "2":
            return [("1d", chunk[0]), ("1u", chunk[0])]
        if kind == "t":
            return [("side", chunk[0])]
        if kind == "l":
            return [("r", chunk[0])]
        third, side = chunk
        keys = [] if third is None else [("2d", third), ("2u", third)]
        return keys + ([] if side is None else [("own", side, p) for p in range(2)])

    def results(message):
        kind, *chunk = message
        if kind in ("1", "2"):
            return [(kind + "d", chunk[0]), (kind + "u", chunk[0])]
        if kind in ("t", "l"):
            return [(kind, chunk[0])]
        third, side = chunk
        return [("3", third)] if third is not None else [("r", side)]

    def start(message):
        kind, *chunk = message
        inputs = [values[key] for key in sources(message)]
        if kind == "x":
            third, side = chunk
            if third is None:
                inputs = [by_plane(inputs[0], inputs[0], inputs[1], inputs[1])]
            elif side is None:
                inputs = [by_plane(inputs[0], inputs[0], inputs[1], inputs[1])]
            else:
                inputs = [by_plane(inputs[2], inputs[0], inputs[1], inputs[3])]
            kinds = ["x"]
        else:
            kinds = [key[0] for key in results(message)]
        outs = [lax.ppermute(v, "gz", HOPS[k]) for v, k in zip(inputs, kinds)]
        values.update(zip(results(message), outs))
        if kind == "x" and third is not None and side is not None:
            values["r", side] = outs[0]

    def swap(value, axis, bits):
        return lax.ppermute(value, axis, [(i, i ^ bits) for i in range(lax.axis_size(axis))])

    def share(name, g):
        for m in range(1, gx):
            values[name, g, m] = swap(values[name, g, m], "gx", m)

    def pass_on(g):
        for m in range(gx):
            values["other", g, m] = swap(values["right", g, m], "gy", 1)

    def project_right(g):
        names = ("1d", "1u", "2d", "2u", "3", "r")
        arrays = [values["own", g, p] for p in range(2)] + [values[name, g] for name in names]
        slots = (
            ((0, (0, 1)), (1, (2, 3))),
            ((2, (0, 1)), (3, (2, 3))),
            ((4, (0, 1)), (5, (2, 3))),
            ((6, (0, 3)), (7, (1, 2))),
        )
        mask = right_mask[:, g * size : (g + 1) * size]
        outs = project(plane, slots, arrays, mask, right_weight, right_gain, gx, False)
        values.update({("right", g, m): outs[m] for m in range(gx)})

    def project_left(g):
        names = ("1d", "1u", "2d", "2u", "3", "l", "t")
        arrays = [values["own", g, p] for p in range(2)] + [values[name, g] for name in names]
        slots = (
            ((0, (0, 2)), (1, (1, 3))),
            ((2, (0, 2)), (3, (1, 3))),
            ((4, (0,)), (8, (1, 2)), (5, (3,))),
            ((6, (0, 3)), (7, (1, 2))),
        )
        mask = left_mask[:, g * size : (g + 1) * size]
        outs = project(plane, slots, arrays, mask, left_weight, left_gain, gx, True)
        values.update({("left", g, m): outs[m] for m in range(gx)})
        values["normed", g] = outs[gx]

    target = (((x // blocks) ^ y) * blocks + x % blocks) ^ jnp.arange(gx)
    target = target.astype(jnp.int32)

    def multiply(group):
        rights = [values[key, c, m] for key in ("right", "other") for c in range(CHUNKS) for m in range(gx)]
        lefts = [values["left", g, m] for g in group for m in range(gx)]
        outs = product(target, lefts, rights, gx, 2)
        for i, g in enumerate(group):
            values.update({("mixed", g, m): outs[i * gx + m] for m in range(gx)})

    def complete(g):
        mixed = [values["mixed", g, m] for m in range(gx)]
        outs = finish(mixed, values["normed", g], 0, out_weight, gate_weight, mix_gain, gz)
        values.update({("out", g, q): outs[q] for q in range(gz)})
        for q in range(1, gz):
            values["out", g, q] = swap(outs[q], "gz", q)

    def cut(g):
        for p in range(2):
            values["own", g, p] = values["tiles"][:, :, p, g * size : (g + 1) * size]
        values["side", g] = jnp.where(z < 2, values["own", g, 0], values["own", g, 1])

    values["tiles"] = tiles
    values.update({("held", i): array for i, array in enumerate(held)})
    cut(0)
    waits = ["tiles"]
    for e, messages in enumerate(EVENTS):
        keys = [key for message in EVENTS[e - 2] for key in results(message)] if e >= 2 else []
        keys += [key for message in messages for key in sources(message)]
        sync(*keys, *waits)
        waits = []
        for message in messages:
            start(message)
        if e == 0:
            for g in range(1, CHUNKS):
                cut(g)
            waits = [("held", i) for i in range(len(held))]
        if e == 1:
            rows_held = [values["held", i] for i in range(len(held) - 1)] + [values["held", len(held) - 1][None]]
            mine = jnp.concatenate([w.astype(F32) for w in rows_held], axis=0)
            every = jnp.stack([mine] + [swap(mine, "gz", q) for q in range(1, gz)])
            depth = channels * gz
            row_order, col_order = jnp.asarray(ROW_ORDER)[z], jnp.asarray(COL_ORDER)[z]
            head_order = x ^ jnp.arange(gx)
            by_head = jnp.take(every, head_order ^ z, axis=0)

            def columns(blocks_of, i):
                part = blocks_of[:, i * depth : (i + 1) * depth]
                return jnp.swapaxes(part, 1, 2).reshape(-1, depth).astype(BF16)

            def lanes(vector):
                return jnp.broadcast_to(vector[:, None], (vector.shape[0], LANES))

            def pair_weight(gate, linear, order):
                return block_order(jnp.concatenate([columns(by_head, gate), columns(by_head, linear)]), order, 1)

            left_weight, right_weight = pair_weight(0, 1, row_order), pair_weight(2, 3, col_order)
            gate_weight = block_order(columns(every, 4), row_order, 1)
            out_weight = block_order(columns(every, 5), head_order, 1)
            left_gain, right_gain = (lanes(block_order(in_gain, order, 0)) for order in (row_order, col_order))
            mix_gain = lanes(by_head[:, -1].reshape(-1))
        for name, g in TASKS.get(e, ()):
            if name == "pass":
                pass_on(g)
            else:
                (project_right if name == "right" else project_left)(g)
                share(name, g)
                waits.append((name, g, 0))
        for name, g in TASKS.get(e + 1, ()):
            if name == "pass":
                waits += [("right", g, m) for m in range(gx)]
        for name, g in TASKS.get(e - 1, ()):
            if name == "pass":
                waits += [("other", g, m) for m in range(gx)]

    last = CHUNKS - 1
    sync(*waits, *[key for event in EVENTS[-2:] for message in event for key in results(message)])
    project_left(last)
    sync(("left", last, 0), *[("right", last - 1, m) for m in range(gx)])
    pass_on(last - 1)
    sync(*[(name, g, m) for name, g in (("other", last - 1), ("right", last)) for m in range(gx)])
    pass_on(last)
    previous = None
    for step, g in TAIL:
        needs = {"multiply": ["left"], "complete": ["mixed"], "share": ["left"]}[step]
        group = g if step == "multiply" else (g,)
        keys = [(name, c, m) for name in needs for c in group for m in range(gx)]
        if step == "complete" and g >= 2:
            keys += [("out", g - 2, q) for q in range(gz)]
        sync(*keys, *([previous] if previous else []))
        if step == "multiply":
            multiply(group)
            previous = ("mixed", group[0], 0)
            for c in group:
                share("mixed", c)
        elif step == "share":
            share("left", g)
        else:
            complete(g)
            previous = ("out", g, 0)
    update = None
    for g in range(0, CHUNKS):
        update = assemble(plane, [values["out", g, q] for q in range(gz)], gz, g, CHUNKS, update)
    return update.reshape(pair.shape)


def plain_local(
    pair,
    pair_mask,
    in_gain,
    w_left,
    w_left_gate,
    w_right,
    w_right_gate,
    w_out_gate,
    out_gain,
    w_out,
):
    gathered = lax.all_gather(pair, "gz", axis=0, tiled=True).astype(F32)
    average = jnp.mean(gathered, axis=0)
    centered = gathered - average
    spread = jnp.mean(jnp.square(centered), axis=0)
    normed = (centered * lax.rsqrt(spread + epsilon) * in_gain[:, None, None]).astype(BF16)
    mask_float = pair_mask.astype(F32)[None]

    def project_all(weight):
        return jnp.einsum("cik,ch->hik", normed, weight, preferred_element_type=F32)

    left_rows = (mask_float * jax.nn.sigmoid(project_all(w_left_gate)) * project_all(w_left)).astype(BF16)
    right_rows = (mask_float * jax.nn.sigmoid(project_all(w_right_gate)) * project_all(w_right)).astype(BF16)
    out_gate = jax.nn.sigmoid(jnp.einsum("cij,cd->dij", normed, w_out_gate, preferred_element_type=F32))
    left_group, right_group = (
        lax.all_to_all(left_rows, "gx", split_axis=0, concat_axis=2, tiled=True),
        lax.all_to_all(right_rows, "gx", split_axis=0, concat_axis=2, tiled=True),
    )
    full_product = lax.dot_general(
        left_group,
        lax.all_gather(right_group, "gy", axis=1, tiled=True),
        (((2,), (2,)), ((0,), (0,))),
        preferred_element_type=F32,
    )
    mixed_sum = lax.all_to_all(full_product, "gx", split_axis=2, concat_axis=0, tiled=True)
    channel_count = lax.axis_size("gz") * mixed_sum.shape[0]
    mix_average = lax.psum(jnp.sum(mixed_sum, axis=0), "gz") / channel_count
    mix_centered = mixed_sum - mix_average
    mix_spread = lax.psum(jnp.sum(jnp.square(mix_centered), axis=0), "gz") / channel_count
    local_mix = (mix_centered * lax.rsqrt(mix_spread + epsilon) * out_gain[:, None, None]).astype(BF16)
    normed_mix = lax.all_gather(local_mix, "gz", axis=0, tiled=True)
    projected = jnp.einsum("hij,hd->dij", normed_mix, w_out, preferred_element_type=F32)
    return (out_gate * projected).astype(BF16)


def solution(mesh):
    placed = (
        P("gz", "gy", "gx"),
        P("gy", "gx"),
        P(),
        P(None, "gz"),
        P(None, "gz"),
        P(None, "gz"),
        P(None, "gz"),
        P(None, "gz"),
        P("gz"),
        P(None, "gz"),
    )
    fits = mesh.shape["gx"] == 4 and mesh.shape["gy"] == 2 and mesh.shape["gz"] == 4

    def step(*args):
        return local(*args) if fits else plain_local(*args)

    step = jax.shard_map(step, mesh=mesh, in_specs=placed, out_specs=P("gz", "gy", "gx"), check_vma=False)
    return step
```

```python
import functools

import jax
import jax.numpy as jnp
from jax import lax
from jax.experimental import pallas as pl
from jax.experimental.pallas import tpu as pltpu
from jax.sharding import PartitionSpec as P


epsilon = 1e-05
CHUNKS = 4
ROWS = 16
PITCH = 24
LANES = 128
F32, BF16 = jnp.float32, jnp.bfloat16
ARBITRARY = pltpu.GridDimensionSemantics.ARBITRARY

ROW_ORDER = ((0, 1, 2, 3), (1, 0, 2, 3), (2, 3, 1, 0), (3, 2, 1, 0))
COL_ORDER = ((0, 1, 2, 3), (1, 2, 3, 0), (2, 1, 0, 3), (3, 2, 1, 0))

HOPS = {
    "1d": ((3, 2), (2, 1), (1, 0)),
    "1u": ((0, 1), (1, 2), (2, 3)),
    "2d": ((2, 1), (1, 0)),
    "2u": ((1, 2), (2, 3)),
    "x": ((0, 1), (1, 0), (2, 3), (3, 2)),
    "t": ((0, 0), (1, 2), (2, 1), (3, 3)),
    "l": ((0, 0), (1, 2), (2, 1), (3, 3)),
}
EVENTS = (
    (("1", 0),),
    (("x", None, 0), ("t", 0)),
    (("2", 0),),
    (("1", 1),),
    (("l", 0), ("x", 0, 1)),
    (("2", 1),),
    (("1", 2),),
    (("t", 1), ("x", 1, 2)),
    (("2", 2),),
    (("1", 3),),
    (("l", 1), ("x", 2, 3)),
    (("2", 3),),
    (("t", 2),),
    (("l", 2), ("x", 3, None)),
    (("t", 3),),
    (("l", 3),),
)
AHEAD = {6: (("right", 0),)}
TASKS = {
    7: (("left", 0),),
    9: (("right", 1),),
    10: (("pass", 0),),
    12: (("right", 2),),
    13: (("left", 1),),
    14: (("pass", 1),),
    15: (("right", 3), ("left", 2)),
}
TAIL = (
    ("multiply", (0, 1)),
    ("complete", 0),
    ("multiply", (2,)),
    ("share", 3),
    ("complete", 1),
    ("complete", 2),
    ("multiply", (3,)),
    ("complete", 3),
)


def sigmoid(x):
    return 1.0 / (1.0 + jnp.exp(-x))


def norm_channels(x, gain):
    average = jnp.mean(x, axis=0, keepdims=True)
    centered = x - average
    spread = jnp.mean(jnp.square(centered), axis=0, keepdims=True)
    return (centered * lax.rsqrt(spread + epsilon) * gain).astype(BF16)


def dot(a, b, dims=(((1,), (0,)), ((), ()))):
    return lax.dot_general(a, b, dims, preferred_element_type=F32)


def project_kernel(slots, emit, parts, plane_ref, *refs):
    n_in = sum(len(slot) for slot in slots)
    ins = refs[:n_in]
    mask_ref, weight_ref, gain_ref = refs[n_in : n_in + 3]
    outs = refs[n_in + 3 : n_in + 3 + parts + (1 if emit else 0)]
    x_ref, y_ref = refs[-2:]
    plane = plane_ref[0]
    width = ins[0].shape[-1]
    halves = width // LANES
    channels = ins[0].shape[0]
    position = 0
    for slot_index, slot in enumerate(slots):
        base = slot_index * channels
        for planes in slot:
            source = ins[position]
            position += 1
            hit = functools.reduce(jnp.logical_or, [plane == p for p in planes])

            @pl.when(hit)
            def _(source=source, base=base):
                for half in range(halves):
                    block = source[:, 0, :, half * LANES : (half + 1) * LANES].astype(F32)
                    x_ref[half, base : base + channels, 0:ROWS, :] = block

    total = len(slots) * channels
    hidden = weight_ref.shape[0] // 2
    x_flat = x_ref.reshape(halves, total * PITCH, LANES)
    y_flat = y_ref.reshape(halves, hidden * PITCH, LANES)
    gain = gain_ref[...]

    def step(row, carry):
        normed = [
            norm_channels(x_flat[half, pl.ds(row, total, stride=PITCH), :], gain) for half in range(halves)
        ]
        if emit:
            upper = (plane >> 1) == 1
            chosen = jnp.where(upper, normed[1].astype(F32), normed[0].astype(F32))
            outs[parts][0, row] = chosen.astype(BF16)
        both = dot(weight_ref[...], jnp.concatenate(normed, axis=1))
        mask = mask_ref[0, pl.ds(row, 1), :]
        value = mask * sigmoid(both[:hidden]) * both[hidden:]
        for half in range(halves):
            y_flat[half, pl.ds(row, hidden, stride=PITCH), :] = value[:, half * LANES : (half + 1) * LANES]
        return carry

    lax.fori_loop(0, ROWS, step, 0, unroll=8)
    part = hidden // parts
    for m in range(parts):
        for half in range(halves):
            block = y_ref[half, m * part : (m + 1) * part, 0:ROWS, :]
            outs[m][:, 0, :, half * LANES : (half + 1) * LANES] = block.astype(BF16)


def project(plane, slots, arrays, mask, weight, gain, parts, emit):
    channels, blocks, size, width = arrays[0].shape
    hidden = weight.shape[0] // 2
    total = len(slots) * channels
    planes = tuple(tuple(p for _, p in slot) for slot in slots)
    ins = [arrays[index] for slot in slots for index, _ in slot]
    block = pl.BlockSpec((channels, 1, ROWS, width), lambda n, t: (0, n, t, 0))
    whole = lambda n, t: (0, 0)
    out_specs = [pl.BlockSpec((hidden // parts, 1, ROWS, width), lambda n, t: (0, n, t, 0))] * parts
    out_shape = [jax.ShapeDtypeStruct((hidden // parts, blocks, size, width), BF16)] * parts
    if emit:
        out_specs = out_specs + [pl.BlockSpec((1, ROWS, total, LANES), lambda n, t: (n, t, 0, 0))]
        out_shape = out_shape + [jax.ShapeDtypeStruct((blocks, size, total, LANES), BF16)]
    pixels = blocks * size * width
    return pl.pallas_call(
        functools.partial(project_kernel, planes, emit, parts),
        grid=(blocks, size // ROWS),
        in_specs=[pl.BlockSpec(memory_space=pltpu.SMEM)]
        + [block] * len(ins)
        + [
            pl.BlockSpec((1, ROWS, width), lambda n, t: (n, t, 0)),
            pl.BlockSpec(weight.shape, whole),
            pl.BlockSpec(gain.shape, whole),
        ],
        out_specs=out_specs,
        out_shape=out_shape,
        scratch_shapes=[
            pltpu.VMEM((width // LANES, total, PITCH, LANES), F32),
            pltpu.VMEM((width // LANES, hidden, PITCH, LANES), F32),
        ],
        compiler_params=pltpu.CompilerParams(dimension_semantics=(ARBITRARY, ARBITRARY)),
        cost_estimate=pl.CostEstimate(
            flops=16 * pixels * total * hidden, bytes_accessed=2 * pixels * (total * 3 + hidden), transcendentals=0
        ),
        name="project",
    )(plane, *ins, mask, weight, gain)


def product_kernel(parts, chunks, left_chunks, target_ref, *refs):
    lefts = refs[: left_chunks * parts]
    rights = refs[left_chunks * parts : (left_chunks + 2 * chunks) * parts]
    outs = refs[(left_chunks + 2 * chunks) * parts :]
    heads, blocks, size, _ = lefts[0].shape
    cores = 2
    for head in range(heads):
        rows = [
            jnp.concatenate([lefts[c * parts + m][head, n] for m in range(parts)], axis=1)
            for c in range(left_chunks)
            for n in range(blocks)
        ]
        left = jnp.concatenate(rows, axis=0)
        rows = [
            jnp.concatenate([rights[(core * chunks + g) * parts + m][head, n] for m in range(parts)], axis=1)
            for core in range(cores)
            for n in range(blocks)
            for g in range(chunks)
        ]
        right = jnp.concatenate(rows, axis=0)
        mixed = dot(left, right, (((1,), (1,)), ((), ())))
        span = chunks * size
        pieces = [mixed[:, p * span : (p + 1) * span] for p in range(cores * blocks)]
        for m in range(parts):
            pick = target_ref[m]
            value = pieces[0]
            for p in range(1, len(pieces)):
                value = jnp.where(pick == p, pieces[p], value)
            value = value.astype(BF16)
            for c in range(left_chunks):
                rows = blocks * size
                outs[c * parts + m][head] = value[c * rows : (c + 1) * rows].reshape(blocks, size, span)


def product(target, lefts, rights, parts, heads):
    hidden, blocks, size, width = lefts[0].shape
    cores = 2
    chunks, left_chunks = len(rights) // (cores * parts), len(lefts) // parts
    span = chunks * size
    left_block = pl.BlockSpec((heads, blocks, size, width), lambda h: (h, 0, 0, 0))
    rows = left_chunks * blocks * size
    return pl.pallas_call(
        functools.partial(product_kernel, parts, chunks, left_chunks),
        grid=(hidden // heads,),
        in_specs=[pl.BlockSpec(memory_space=pltpu.SMEM)] + [left_block] * (len(lefts) + len(rights)),
        out_specs=[pl.BlockSpec((heads, blocks, size, span), lambda h: (h, 0, 0, 0))] * len(lefts),
        out_shape=[jax.ShapeDtypeStruct((hidden, blocks, size, span), BF16)] * len(lefts),
        compiler_params=pltpu.CompilerParams(dimension_semantics=(ARBITRARY,)),
        cost_estimate=pl.CostEstimate(
            flops=2 * hidden * rows * (cores * blocks * span) * width * parts,
            bytes_accessed=2 * hidden * width * parts * (rows + cores * blocks * span),
            transcendentals=0,
        ),
        name="product",
    )(target, *lefts, *rights)


def finish_kernel(parts, *refs):
    mixed = refs[:parts]
    normed_ref, out_ref, gate_ref, gain_ref = refs[parts : parts + 4]
    outs = refs[parts + 4 : -2]
    x_ref, y_ref = refs[-2:]
    part = mixed[0].shape[0]
    for m in range(parts):
        x_ref[m * part : (m + 1) * part, 0:ROWS, :] = mixed[m][:, 0].astype(F32)
    total = parts * part
    x_flat = x_ref.reshape(total * PITCH, LANES)
    y_flat = y_ref.reshape(out_ref.shape[0] * PITCH, LANES)
    gain = gain_ref[...]
    together = 2

    def step(pair, carry):
        base = pair * together
        normed = [
            norm_channels(x_flat[pl.ds(base + r, total, stride=PITCH), :], gain) for r in range(together)
        ]
        gates = dot(gate_ref[...], jnp.concatenate([normed_ref[0, base + r] for r in range(together)], axis=1))
        value = sigmoid(gates) * dot(out_ref[...], jnp.concatenate(normed, axis=1))
        for r in range(together):
            y_flat[pl.ds(base + r, value.shape[0], stride=PITCH), :] = value[:, r * LANES : (r + 1) * LANES]
        return carry

    lax.fori_loop(0, ROWS // together, step, 0, unroll=4)
    part = out_ref.shape[0] // len(outs)
    for q, out in enumerate(outs):
        block = y_ref[q * part : (q + 1) * part, 0:ROWS, :]
        out[:, 0] = block.astype(BF16)


def finish(mixed, normed, offset, w_out, w_gate, gain, planes):
    part, width = mixed[0].shape[0], mixed[0].shape[-1]
    blocks, size = normed.shape[:2]
    first = offset // ROWS
    depth = w_out.shape[0]
    total = part * len(mixed)
    whole = lambda n, t: (0, 0)
    pixels = blocks * size * width
    return pl.pallas_call(
        functools.partial(finish_kernel, len(mixed)),
        grid=(blocks, size // ROWS),
        in_specs=[pl.BlockSpec((part, 1, ROWS, width), lambda n, t: (0, n, t + first, 0))] * len(mixed)
        + [
            pl.BlockSpec((1, ROWS, normed.shape[2], width), lambda n, t: (n, t, 0, 0)),
            pl.BlockSpec(w_out.shape, whole),
            pl.BlockSpec(w_gate.shape, whole),
            pl.BlockSpec(gain.shape, whole),
        ],
        out_specs=[pl.BlockSpec((depth // planes, 1, ROWS, width), lambda n, t: (0, n, t, 0))] * planes,
        out_shape=[jax.ShapeDtypeStruct((depth // planes, blocks, size, width), BF16)] * planes,
        scratch_shapes=[pltpu.VMEM((total, PITCH, width), F32), pltpu.VMEM((depth, PITCH, width), F32)],
        compiler_params=pltpu.CompilerParams(dimension_semantics=(ARBITRARY, ARBITRARY)),
        cost_estimate=pl.CostEstimate(
            flops=16 * pixels * total * depth, bytes_accessed=2 * pixels * total * 3, transcendentals=0
        ),
        name="finish",
    )(*mixed, normed, w_out, w_gate, gain)


def assemble_kernel(planes, chunks, plane_ref, *refs):
    ins, out = refs[: planes * chunks], refs[-1]
    plane = plane_ref[0]
    size = ins[0].shape[2]
    for mine in range(planes):

        @pl.when(plane == mine)
        def _(mine=mine):
            for source in range(planes):
                a, b = source & 1, source >> 1
                for g in range(chunks):
                    out[:, 0, a, g * size : (g + 1) * size, b * LANES : (b + 1) * LANES] = ins[
                        (source ^ mine) * chunks + g
                    ][:, 0]


def assemble(plane, pieces, planes, position, count, base=None):
    chunks = len(pieces) // planes
    depth, blocks, size, width = pieces[0].shape
    step = depth // 2
    out_block = (step, 1, 2, chunks * size, 2 * width)
    return pl.pallas_call(
        functools.partial(assemble_kernel, planes, chunks),
        grid=(depth // step, blocks),
        in_specs=[pl.BlockSpec(memory_space=pltpu.SMEM)]
        + [pl.BlockSpec((step, 1, size, width), lambda d, n: (d, n, 0, 0))] * len(pieces)
        + ([] if base is None else [pl.BlockSpec(memory_space=pl.ANY)]),
        out_specs=pl.BlockSpec(out_block, lambda d, n: (d, n, 0, position // chunks, 0)),
        out_shape=jax.ShapeDtypeStruct((depth, blocks, 2, count * size, 2 * width), BF16),
        input_output_aliases={} if base is None else {1 + len(pieces): 0},
        compiler_params=pltpu.CompilerParams(dimension_semantics=(ARBITRARY, ARBITRARY)),
        cost_estimate=pl.CostEstimate(
            flops=4 * depth * blocks * size * width * len(pieces),
            bytes_accessed=4 * depth * blocks * size * width * len(pieces),
            transcendentals=0,
        ),
        name="assemble",
    )(plane, *pieces, *(() if base is None else (base,)))


def block_order(array, order, axis):
    split = array.shape[:axis] + (order.shape[0], array.shape[axis] // order.shape[0]) + array.shape[axis + 1 :]
    return jnp.take(array.reshape(split), order, axis=axis).reshape(array.shape)


def local(
    pair,
    pair_mask,
    in_gain,
    w_left,
    w_left_gate,
    w_right,
    w_right_gate,
    w_out_gate,
    out_gain,
    w_out,
):
    gx, gz = lax.axis_size("gx"), lax.axis_size("gz")
    x, y, z = lax.axis_index("gx"), lax.axis_index("gy"), lax.axis_index("gz")
    plane = z.astype(jnp.int32).reshape(1)
    channels, rows, width = pair.shape
    span = width // 2
    blocks = rows // (2 * span)
    size = span // CHUNKS
    tiles = pair.reshape(channels, blocks, 2, span, width)
    masks = pair_mask.astype(F32).reshape(blocks, 2, span, width)
    left_mask = lax.dynamic_index_in_dim(masks, z & 1, 1, keepdims=False)
    right_mask = lax.dynamic_index_in_dim(masks, z >> 1, 1, keepdims=False)
    held = (w_left_gate, w_left, w_right_gate, w_right, w_out_gate, w_out, out_gain)

    values = {}

    def sync(*keys):
        keys = list(dict.fromkeys(keys))
        values.update(zip(keys, lax.optimization_barrier(tuple(values[key] for key in keys))))

    def by_plane(*choices):
        value = choices[-1]
        for p, choice in list(enumerate(choices))[-2::-1]:
            value = jnp.where(z == p, choice, value)
        return value

    def sources(message):
        kind, *chunk = message
        if kind == "1":
            return [("own", chunk[0], p) for p in range(2)]
        if kind == "2":
            return [("1d", chunk[0]), ("1u", chunk[0])]
        if kind == "t":
            return [("side", chunk[0])]
        if kind == "l":
            return [("r", chunk[0])]
        third, side = chunk
        keys = [] if third is None else [("2d", third), ("2u", third)]
        return keys + ([] if side is None else [("own", side, p) for p in range(2)])

    def results(message):
        kind, *chunk = message
        if kind in ("1", "2"):
            return [(kind + "d", chunk[0]), (kind + "u", chunk[0])]
        if kind in ("t", "l"):
            return [(kind, chunk[0])]
        third, side = chunk
        return [("3", third)] if third is not None else [("r", side)]

    def start(message):
        kind, *chunk = message
        inputs = [values[key] for key in sources(message)]
        if kind == "x":
            third, side = chunk
            if third is None:
                inputs = [by_plane(inputs[0], inputs[0], inputs[1], inputs[1])]
            elif side is None:
                inputs = [by_plane(inputs[0], inputs[0], inputs[1], inputs[1])]
            else:
                inputs = [by_plane(inputs[2], inputs[0], inputs[1], inputs[3])]
            kinds = ["x"]
        else:
            kinds = [key[0] for key in results(message)]
        outs = [lax.ppermute(v, "gz", HOPS[k]) for v, k in zip(inputs, kinds)]
        values.update(zip(results(message), outs))
        if kind == "x" and third is not None and side is not None:
            values["r", side] = outs[0]

    def swap(value, axis, bits):
        return lax.ppermute(value, axis, [(i, i ^ bits) for i in range(lax.axis_size(axis))])

    def share(name, g):
        for m in range(1, gx):
            values[name, g, m] = swap(values[name, g, m], "gx", m)

    def pass_on(g):
        for m in range(gx):
            values["other", g, m] = swap(values["right", g, m], "gy", 1)

    def project_right(g):
        names = ("1d", "1u", "2d", "2u", "3", "r")
        arrays = [values["own", g, p] for p in range(2)] + [values[name, g] for name in names]
        slots = (
            ((0, (0, 1)), (1, (2, 3))),
            ((2, (0, 1)), (3, (2, 3))),
            ((4, (0, 1)), (5, (2, 3))),
            ((6, (0, 3)), (7, (1, 2))),
        )
        mask = right_mask[:, g * size : (g + 1) * size]
        outs = project(plane, slots, arrays, mask, right_weight, right_gain, gx, False)
        values.update({("right", g, m): outs[m] for m in range(gx)})

    def project_left(g):
        names = ("1d", "1u", "2d", "2u", "3", "l", "t")
        arrays = [values["own", g, p] for p in range(2)] + [values[name, g] for name in names]
        slots = (
            ((0, (0, 2)), (1, (1, 3))),
            ((2, (0, 2)), (3, (1, 3))),
            ((4, (0,)), (8, (1, 2)), (5, (3,))),
            ((6, (0, 3)), (7, (1, 2))),
        )
        mask = left_mask[:, g * size : (g + 1) * size]
        outs = project(plane, slots, arrays, mask, left_weight, left_gain, gx, True)
        values.update({("left", g, m): outs[m] for m in range(gx)})
        values["normed", g] = outs[gx]

    target = (((x // blocks) ^ y) * blocks + x % blocks) ^ jnp.arange(gx)
    target = target.astype(jnp.int32)

    def multiply(group):
        rights = [values[key, c, m] for key in ("right", "other") for c in range(CHUNKS) for m in range(gx)]
        lefts = [values["left", g, m] for g in group for m in range(gx)]
        outs = product(target, lefts, rights, gx, 4)
        for i, g in enumerate(group):
            values.update({("mixed", g, m): outs[i * gx + m] for m in range(gx)})

    def complete(g):
        mixed = [values["mixed", g, m] for m in range(gx)]
        outs = finish(mixed, values["normed", g], 0, out_weight, gate_weight, mix_gain, gz)
        values.update({("out", g, q): outs[q] for q in range(gz)})
        for q in range(1, gz):
            values["out", g, q] = swap(outs[q], "gz", q)

    def cut(g):
        for p in range(2):
            values["own", g, p] = values["tiles"][:, :, p, g * size : (g + 1) * size]
        values["side", g] = jnp.where(z < 2, values["own", g, 0], values["own", g, 1])

    values["tiles"] = tiles
    values.update({("held", i): array for i, array in enumerate(held)})
    cut(0)
    waits = ["tiles"]
    for e, messages in enumerate(EVENTS):
        keys = [key for message in EVENTS[e - 2] for key in results(message)] if e >= 2 else []
        keys += [key for message in messages for key in sources(message)]
        sync(*keys, *waits)
        waits = []
        for name, g in AHEAD.get(e, ()):
            (project_right if name == "right" else project_left)(g)
            share(name, g)
            keys = [(name, g, 0)] + [key for message in messages for key in sources(message)]
            sync(*keys)
        for message in messages:
            start(message)
        if e == 0:
            for g in range(1, CHUNKS):
                cut(g)
            waits = [("held", i) for i in range(len(held))]
        if e == 1:
            rows_held = [values["held", i] for i in range(len(held) - 1)] + [values["held", len(held) - 1][None]]
            mine = jnp.concatenate([w.astype(F32) for w in rows_held], axis=0)
            every = jnp.stack([mine] + [swap(mine, "gz", q) for q in range(1, gz)])
            depth = channels * gz
            row_order, col_order = jnp.asarray(ROW_ORDER)[z], jnp.asarray(COL_ORDER)[z]
            head_order = x ^ jnp.arange(gx)
            by_head = jnp.take(every, head_order ^ z, axis=0)

            def columns(blocks_of, i):
                part = blocks_of[:, i * depth : (i + 1) * depth]
                return jnp.swapaxes(part, 1, 2).reshape(-1, depth).astype(BF16)

            def lanes(vector):
                return jnp.broadcast_to(vector[:, None], (vector.shape[0], LANES))

            def pair_weight(gate, linear, order):
                return block_order(jnp.concatenate([columns(by_head, gate), columns(by_head, linear)]), order, 1)

            left_weight, right_weight = pair_weight(0, 1, row_order), pair_weight(2, 3, col_order)
            gate_weight = block_order(columns(every, 4), row_order, 1)
            out_weight = block_order(columns(every, 5), head_order, 1)
            left_gain, right_gain = (lanes(block_order(in_gain, order, 0)) for order in (row_order, col_order))
            mix_gain = lanes(by_head[:, -1].reshape(-1))
        for name, g in TASKS.get(e, ()):
            if name == "pass":
                pass_on(g)
            else:
                (project_right if name == "right" else project_left)(g)
                share(name, g)
                waits.append((name, g, 0))
        for name, g in TASKS.get(e + 1, ()):
            if name == "pass":
                waits += [("right", g, m) for m in range(gx)]
        for name, g in TASKS.get(e - 1, ()):
            if name == "pass":
                waits += [("other", g, m) for m in range(gx)]

    last = CHUNKS - 1
    sync(*waits, *[key for event in EVENTS[-2:] for message in event for key in results(message)])
    project_left(last)
    sync(("left", last, 0), *[("right", last - 1, m) for m in range(gx)])
    pass_on(last - 1)
    sync(*[(name, g, m) for name, g in (("other", last - 1), ("right", last)) for m in range(gx)])
    pass_on(last)
    previous = None
    for step, g in TAIL:
        needs = {"multiply": ["left"], "complete": ["mixed"], "share": ["left"]}[step]
        group = g if step == "multiply" else (g,)
        keys = [(name, c, m) for name in needs for c in group for m in range(gx)]
        sync(*keys, *([previous] if previous else []))
        if step == "multiply":
            multiply(group)
            previous = ("mixed", group[0], 0)
            for c in group:
                share("mixed", c)
        elif step == "share":
            share("left", g)
        else:
            complete(g)
            previous = ("out", g, 0)
    update = None
    for g in range(0, CHUNKS):
        update = assemble(plane, [values["out", g, q] for q in range(gz)], gz, g, CHUNKS, update)
    return update.reshape(pair.shape)


def plain_local(
    pair,
    pair_mask,
    in_gain,
    w_left,
    w_left_gate,
    w_right,
    w_right_gate,
    w_out_gate,
    out_gain,
    w_out,
):
    gathered = lax.all_gather(pair, "gz", axis=0, tiled=True).astype(F32)
    average = jnp.mean(gathered, axis=0)
    centered = gathered - average
    spread = jnp.mean(jnp.square(centered), axis=0)
    normed = (centered * lax.rsqrt(spread + epsilon) * in_gain[:, None, None]).astype(BF16)
    mask_float = pair_mask.astype(F32)[None]

    def project_all(weight):
        return jnp.einsum("cik,ch->hik", normed, weight, preferred_element_type=F32)

    left_rows = (mask_float * jax.nn.sigmoid(project_all(w_left_gate)) * project_all(w_left)).astype(BF16)
    right_rows = (mask_float * jax.nn.sigmoid(project_all(w_right_gate)) * project_all(w_right)).astype(BF16)
    out_gate = jax.nn.sigmoid(jnp.einsum("cij,cd->dij", normed, w_out_gate, preferred_element_type=F32))
    left_group, right_group = (
        lax.all_to_all(left_rows, "gx", split_axis=0, concat_axis=2, tiled=True),
        lax.all_to_all(right_rows, "gx", split_axis=0, concat_axis=2, tiled=True),
    )
    full_product = lax.dot_general(
        left_group,
        lax.all_gather(right_group, "gy", axis=1, tiled=True),
        (((2,), (2,)), ((0,), (0,))),
        preferred_element_type=F32,
    )
    mixed_sum = lax.all_to_all(full_product, "gx", split_axis=2, concat_axis=0, tiled=True)
    channel_count = lax.axis_size("gz") * mixed_sum.shape[0]
    mix_average = lax.psum(jnp.sum(mixed_sum, axis=0), "gz") / channel_count
    mix_centered = mixed_sum - mix_average
    mix_spread = lax.psum(jnp.sum(jnp.square(mix_centered), axis=0), "gz") / channel_count
    local_mix = (mix_centered * lax.rsqrt(mix_spread + epsilon) * out_gain[:, None, None]).astype(BF16)
    normed_mix = lax.all_gather(local_mix, "gz", axis=0, tiled=True)
    projected = jnp.einsum("hij,hd->dij", normed_mix, w_out, preferred_element_type=F32)
    return (out_gate * projected).astype(BF16)


def solution(mesh):
    placed = (
        P("gz", "gy", "gx"),
        P("gy", "gx"),
        P(),
        P(None, "gz"),
        P(None, "gz"),
        P(None, "gz"),
        P(None, "gz"),
        P(None, "gz"),
        P("gz"),
        P(None, "gz"),
    )
    fits = mesh.shape["gx"] == 4 and mesh.shape["gy"] == 2 and mesh.shape["gz"] == 4

    def step(*args):
        return local(*args) if fits else plain_local(*args)

    step = jax.shard_map(step, mesh=mesh, in_specs=placed, out_specs=P("gz", "gy", "gx"), check_vma=False)
    return step
```

```python
import functools

import jax
import jax.numpy as jnp
from jax import lax
from jax.experimental import pallas as pl
from jax.experimental.pallas import tpu as pltpu
from jax.sharding import PartitionSpec as P


epsilon = 1e-05
CHUNKS = 4
ROWS = 16
PITCH = 24
LANES = 128
F32, BF16 = jnp.float32, jnp.bfloat16
ARBITRARY = pltpu.GridDimensionSemantics.ARBITRARY

ROW_ORDER = ((0, 1, 2, 3), (1, 0, 2, 3), (2, 3, 1, 0), (3, 2, 1, 0))
COL_ORDER = ((0, 1, 2, 3), (1, 2, 3, 0), (2, 1, 0, 3), (3, 2, 1, 0))

HOPS = {
    "1d": ((3, 2), (2, 1), (1, 0)),
    "1u": ((0, 1), (1, 2), (2, 3)),
    "2d": ((2, 1), (1, 0)),
    "2u": ((1, 2), (2, 3)),
    "x": ((0, 1), (1, 0), (2, 3), (3, 2)),
    "t": ((0, 0), (1, 2), (2, 1), (3, 3)),
    "l": ((0, 0), (1, 2), (2, 1), (3, 3)),
}
EVENTS = (
    (("1", 0),),
    (("x", None, 0), ("t", 0)),
    (("2", 0),),
    (("1", 1),),
    (("l", 0), ("x", 0, 1)),
    (("2", 1),),
    (("1", 2),),
    (("t", 1), ("x", 1, 2)),
    (("2", 2),),
    (("1", 3),),
    (("l", 1), ("x", 2, 3)),
    (("2", 3),),
    (("t", 2),),
    (("l", 2), ("x", 3, None)),
    (("t", 3),),
    (("l", 3),),
)
AHEAD = {6: (("right", 0),)}
TASKS = {
    7: (("left", 0),),
    9: (("right", 1),),
    10: (("pass", 0),),
    12: (("right", 2),),
    13: (("left", 1),),
    14: (("pass", 1),),
    15: (("right", 3), ("early", 3), ("left", 2)),
}
TAIL = (
    ("multiply", (0, 1)),
    ("complete", 0),
    ("multiply", (2,)),
    ("share", 3),
    ("complete", 1),
    ("complete", 2),
    ("multiply", (3,)),
    ("complete", 3),
)


def sigmoid(x):
    return 1.0 / (1.0 + jnp.exp(-x))


def norm_channels(x, gain):
    average = jnp.mean(x, axis=0, keepdims=True)
    centered = x - average
    spread = jnp.mean(jnp.square(centered), axis=0, keepdims=True)
    return (centered * lax.rsqrt(spread + epsilon) * gain).astype(BF16)


def dot(a, b, dims=(((1,), (0,)), ((), ()))):
    return lax.dot_general(a, b, dims, preferred_element_type=F32)


def project_kernel(slots, emit, parts, plane_ref, *refs):
    n_in = sum(len(slot) for slot in slots)
    ins = refs[:n_in]
    mask_ref, weight_ref, gain_ref = refs[n_in : n_in + 3]
    outs = refs[n_in + 3 : n_in + 3 + parts + (1 if emit else 0)]
    x_ref, y_ref = refs[-2:]
    plane = plane_ref[0]
    width = ins[0].shape[-1]
    halves = width // LANES
    channels = ins[0].shape[0]
    position = 0
    for slot_index, slot in enumerate(slots):
        base = slot_index * channels
        for planes in slot:
            source = ins[position]
            position += 1
            hit = functools.reduce(jnp.logical_or, [plane == p for p in planes])

            @pl.when(hit)
            def _(source=source, base=base):
                for half in range(halves):
                    block = source[:, 0, :, half * LANES : (half + 1) * LANES].astype(F32)
                    x_ref[half, base : base + channels, 0:ROWS, :] = block

    total = len(slots) * channels
    hidden = weight_ref.shape[0] // 2
    x_flat = x_ref.reshape(halves, total * PITCH, LANES)
    y_flat = y_ref.reshape(halves, hidden * PITCH, LANES)
    gain = gain_ref[...]

    def step(row, carry):
        normed = [
            norm_channels(x_flat[half, pl.ds(row, total, stride=PITCH), :], gain) for half in range(halves)
        ]
        if emit:
            upper = (plane >> 1) == 1
            chosen = jnp.where(upper, normed[1].astype(F32), normed[0].astype(F32))
            outs[parts][0, row] = chosen.astype(BF16)
        both = dot(weight_ref[...], jnp.concatenate(normed, axis=1))
        mask = mask_ref[0, pl.ds(row, 1), :]
        value = mask * sigmoid(both[:hidden]) * both[hidden:]
        for half in range(halves):
            y_flat[half, pl.ds(row, hidden, stride=PITCH), :] = value[:, half * LANES : (half + 1) * LANES]
        return carry

    lax.fori_loop(0, ROWS, step, 0, unroll=8)
    part = hidden // parts
    for m in range(parts):
        for half in range(halves):
            block = y_ref[half, m * part : (m + 1) * part, 0:ROWS, :]
            outs[m][:, 0, :, half * LANES : (half + 1) * LANES] = block.astype(BF16)


def project(plane, slots, arrays, mask, weight, gain, parts, emit):
    channels, blocks, size, width = arrays[0].shape
    hidden = weight.shape[0] // 2
    total = len(slots) * channels
    planes = tuple(tuple(p for _, p in slot) for slot in slots)
    ins = [arrays[index] for slot in slots for index, _ in slot]
    block = pl.BlockSpec((channels, 1, ROWS, width), lambda n, t: (0, n, t, 0))
    whole = lambda n, t: (0, 0)
    out_specs = [pl.BlockSpec((hidden // parts, 1, ROWS, width), lambda n, t: (0, n, t, 0))] * parts
    out_shape = [jax.ShapeDtypeStruct((hidden // parts, blocks, size, width), BF16)] * parts
    if emit:
        out_specs = out_specs + [pl.BlockSpec((1, ROWS, total, LANES), lambda n, t: (n, t, 0, 0))]
        out_shape = out_shape + [jax.ShapeDtypeStruct((blocks, size, total, LANES), BF16)]
    pixels = blocks * size * width
    return pl.pallas_call(
        functools.partial(project_kernel, planes, emit, parts),
        grid=(blocks, size // ROWS),
        in_specs=[pl.BlockSpec(memory_space=pltpu.SMEM)]
        + [block] * len(ins)
        + [
            pl.BlockSpec((1, ROWS, width), lambda n, t: (n, t, 0)),
            pl.BlockSpec(weight.shape, whole),
            pl.BlockSpec(gain.shape, whole),
        ],
        out_specs=out_specs,
        out_shape=out_shape,
        scratch_shapes=[
            pltpu.VMEM((width // LANES, total, PITCH, LANES), F32),
            pltpu.VMEM((width // LANES, hidden, PITCH, LANES), F32),
        ],
        compiler_params=pltpu.CompilerParams(dimension_semantics=(ARBITRARY, ARBITRARY)),
        cost_estimate=pl.CostEstimate(
            flops=16 * pixels * total * hidden, bytes_accessed=2 * pixels * (total * 3 + hidden), transcendentals=0
        ),
        name="project",
    )(plane, *ins, mask, weight, gain)


def product_kernel(parts, chunks, left_chunks, target_ref, *refs):
    lefts = refs[: left_chunks * parts]
    rights = refs[left_chunks * parts : (left_chunks + 2 * chunks) * parts]
    outs = refs[(left_chunks + 2 * chunks) * parts :]
    heads, blocks, size, _ = lefts[0].shape
    cores = 2
    for head in range(heads):
        rows = [
            jnp.concatenate([lefts[c * parts + m][head, n] for m in range(parts)], axis=1)
            for c in range(left_chunks)
            for n in range(blocks)
        ]
        left = jnp.concatenate(rows, axis=0)
        rows = [
            jnp.concatenate([rights[(core * chunks + g) * parts + m][head, n] for m in range(parts)], axis=1)
            for core in range(cores)
            for n in range(blocks)
            for g in range(chunks)
        ]
        right = jnp.concatenate(rows, axis=0)
        mixed = dot(left, right, (((1,), (1,)), ((), ())))
        span = chunks * size
        pieces = [mixed[:, p * span : (p + 1) * span] for p in range(cores * blocks)]
        for m in range(parts):
            pick = target_ref[m]
            value = pieces[0]
            for p in range(1, len(pieces)):
                value = jnp.where(pick == p, pieces[p], value)
            value = value.astype(BF16)
            for c in range(left_chunks):
                rows = blocks * size
                outs[c * parts + m][head] = value[c * rows : (c + 1) * rows].reshape(blocks, size, span)


def product(target, lefts, rights, parts, heads):
    hidden, blocks, size, width = lefts[0].shape
    cores = 2
    chunks, left_chunks = len(rights) // (cores * parts), len(lefts) // parts
    span = chunks * size
    left_block = pl.BlockSpec((heads, blocks, size, width), lambda h: (h, 0, 0, 0))
    rows = left_chunks * blocks * size
    return pl.pallas_call(
        functools.partial(product_kernel, parts, chunks, left_chunks),
        grid=(hidden // heads,),
        in_specs=[pl.BlockSpec(memory_space=pltpu.SMEM)] + [left_block] * (len(lefts) + len(rights)),
        out_specs=[pl.BlockSpec((heads, blocks, size, span), lambda h: (h, 0, 0, 0))] * len(lefts),
        out_shape=[jax.ShapeDtypeStruct((hidden, blocks, size, span), BF16)] * len(lefts),
        compiler_params=pltpu.CompilerParams(dimension_semantics=(ARBITRARY,)),
        cost_estimate=pl.CostEstimate(
            flops=2 * hidden * rows * (cores * blocks * span) * width * parts,
            bytes_accessed=2 * hidden * width * parts * (rows + cores * blocks * span),
            transcendentals=0,
        ),
        name="product",
    )(target, *lefts, *rights)


def finish_kernel(parts, *refs):
    mixed = refs[:parts]
    normed_ref, out_ref, gate_ref, gain_ref = refs[parts : parts + 4]
    outs = refs[parts + 4 : -2]
    x_ref, y_ref = refs[-2:]
    part = mixed[0].shape[0]
    for m in range(parts):
        x_ref[m * part : (m + 1) * part, 0:ROWS, :] = mixed[m][:, 0].astype(F32)
    total = parts * part
    x_flat = x_ref.reshape(total * PITCH, LANES)
    y_flat = y_ref.reshape(out_ref.shape[0] * PITCH, LANES)
    gain = gain_ref[...]
    together = 2

    def step(pair, carry):
        base = pair * together
        normed = [
            norm_channels(x_flat[pl.ds(base + r, total, stride=PITCH), :], gain) for r in range(together)
        ]
        gates = dot(gate_ref[...], jnp.concatenate([normed_ref[0, base + r] for r in range(together)], axis=1))
        value = sigmoid(gates) * dot(out_ref[...], jnp.concatenate(normed, axis=1))
        for r in range(together):
            y_flat[pl.ds(base + r, value.shape[0], stride=PITCH), :] = value[:, r * LANES : (r + 1) * LANES]
        return carry

    lax.fori_loop(0, ROWS // together, step, 0, unroll=4)
    part = out_ref.shape[0] // len(outs)
    for q, out in enumerate(outs):
        block = y_ref[q * part : (q + 1) * part, 0:ROWS, :]
        out[:, 0] = block.astype(BF16)


def finish(mixed, normed, offset, w_out, w_gate, gain, planes):
    part, width = mixed[0].shape[0], mixed[0].shape[-1]
    blocks, size = normed.shape[:2]
    first = offset // ROWS
    depth = w_out.shape[0]
    total = part * len(mixed)
    whole = lambda n, t: (0, 0)
    pixels = blocks * size * width
    return pl.pallas_call(
        functools.partial(finish_kernel, len(mixed)),
        grid=(blocks, size // ROWS),
        in_specs=[pl.BlockSpec((part, 1, ROWS, width), lambda n, t: (0, n, t + first, 0))] * len(mixed)
        + [
            pl.BlockSpec((1, ROWS, normed.shape[2], width), lambda n, t: (n, t, 0, 0)),
            pl.BlockSpec(w_out.shape, whole),
            pl.BlockSpec(w_gate.shape, whole),
            pl.BlockSpec(gain.shape, whole),
        ],
        out_specs=[pl.BlockSpec((depth // planes, 1, ROWS, width), lambda n, t: (0, n, t, 0))] * planes,
        out_shape=[jax.ShapeDtypeStruct((depth // planes, blocks, size, width), BF16)] * planes,
        scratch_shapes=[pltpu.VMEM((total, PITCH, width), F32), pltpu.VMEM((depth, PITCH, width), F32)],
        compiler_params=pltpu.CompilerParams(dimension_semantics=(ARBITRARY, ARBITRARY)),
        cost_estimate=pl.CostEstimate(
            flops=16 * pixels * total * depth, bytes_accessed=2 * pixels * total * 3, transcendentals=0
        ),
        name="finish",
    )(*mixed, normed, w_out, w_gate, gain)


def assemble_kernel(planes, chunks, plane_ref, *refs):
    ins, out = refs[: planes * chunks], refs[-1]
    plane = plane_ref[0]
    size = ins[0].shape[2]
    for mine in range(planes):

        @pl.when(plane == mine)
        def _(mine=mine):
            for source in range(planes):
                a, b = source & 1, source >> 1
                for g in range(chunks):
                    out[:, 0, a, g * size : (g + 1) * size, b * LANES : (b + 1) * LANES] = ins[
                        (source ^ mine) * chunks + g
                    ][:, 0]


def assemble(plane, pieces, planes, position, count, base=None):
    chunks = len(pieces) // planes
    depth, blocks, size, width = pieces[0].shape
    step = depth // 2
    out_block = (step, 1, 2, chunks * size, 2 * width)
    return pl.pallas_call(
        functools.partial(assemble_kernel, planes, chunks),
        grid=(depth // step, blocks),
        in_specs=[pl.BlockSpec(memory_space=pltpu.SMEM)]
        + [pl.BlockSpec((step, 1, size, width), lambda d, n: (d, n, 0, 0))] * len(pieces)
        + ([] if base is None else [pl.BlockSpec(memory_space=pl.ANY)]),
        out_specs=pl.BlockSpec(out_block, lambda d, n: (d, n, 0, position // chunks, 0)),
        out_shape=jax.ShapeDtypeStruct((depth, blocks, 2, count * size, 2 * width), BF16),
        input_output_aliases={} if base is None else {1 + len(pieces): 0},
        compiler_params=pltpu.CompilerParams(dimension_semantics=(ARBITRARY, ARBITRARY)),
        cost_estimate=pl.CostEstimate(
            flops=4 * depth * blocks * size * width * len(pieces),
            bytes_accessed=4 * depth * blocks * size * width * len(pieces),
            transcendentals=0,
        ),
        name="assemble",
    )(plane, *pieces, *(() if base is None else (base,)))


def block_order(array, order, axis):
    split = array.shape[:axis] + (order.shape[0], array.shape[axis] // order.shape[0]) + array.shape[axis + 1 :]
    return jnp.take(array.reshape(split), order, axis=axis).reshape(array.shape)


def local(
    pair,
    pair_mask,
    in_gain,
    w_left,
    w_left_gate,
    w_right,
    w_right_gate,
    w_out_gate,
    out_gain,
    w_out,
):
    gx, gz = lax.axis_size("gx"), lax.axis_size("gz")
    x, y, z = lax.axis_index("gx"), lax.axis_index("gy"), lax.axis_index("gz")
    plane = z.astype(jnp.int32).reshape(1)
    channels, rows, width = pair.shape
    span = width // 2
    blocks = rows // (2 * span)
    size = span // CHUNKS
    tiles = pair.reshape(channels, blocks, 2, span, width)
    masks = pair_mask.astype(F32).reshape(blocks, 2, span, width)
    left_mask = lax.dynamic_index_in_dim(masks, z & 1, 1, keepdims=False)
    right_mask = lax.dynamic_index_in_dim(masks, z >> 1, 1, keepdims=False)
    held = (w_left_gate, w_left, w_right_gate, w_right, w_out_gate, w_out, out_gain)

    values = {}

    def sync(*keys):
        keys = list(dict.fromkeys(keys))
        values.update(zip(keys, lax.optimization_barrier(tuple(values[key] for key in keys))))

    def by_plane(*choices):
        value = choices[-1]
        for p, choice in list(enumerate(choices))[-2::-1]:
            value = jnp.where(z == p, choice, value)
        return value

    def sources(message):
        kind, *chunk = message
        if kind == "1":
            return [("own", chunk[0], p) for p in range(2)]
        if kind == "2":
            return [("1d", chunk[0]), ("1u", chunk[0])]
        if kind == "t":
            return [("side", chunk[0])]
        if kind == "l":
            return [("r", chunk[0])]
        third, side = chunk
        keys = [] if third is None else [("2d", third), ("2u", third)]
        return keys + ([] if side is None else [("own", side, p) for p in range(2)])

    def results(message):
        kind, *chunk = message
        if kind in ("1", "2"):
            return [(kind + "d", chunk[0]), (kind + "u", chunk[0])]
        if kind in ("t", "l"):
            return [(kind, chunk[0])]
        third, side = chunk
        return [("3", third)] if third is not None else [("r", side)]

    def start(message):
        kind, *chunk = message
        inputs = [values[key] for key in sources(message)]
        if kind == "x":
            third, side = chunk
            if third is None:
                inputs = [by_plane(inputs[0], inputs[0], inputs[1], inputs[1])]
            elif side is None:
                inputs = [by_plane(inputs[0], inputs[0], inputs[1], inputs[1])]
            else:
                inputs = [by_plane(inputs[2], inputs[0], inputs[1], inputs[3])]
            kinds = ["x"]
        else:
            kinds = [key[0] for key in results(message)]
        outs = [lax.ppermute(v, "gz", HOPS[k]) for v, k in zip(inputs, kinds)]
        values.update(zip(results(message), outs))
        if kind == "x" and third is not None and side is not None:
            values["r", side] = outs[0]

    def swap(value, axis, bits):
        return lax.ppermute(value, axis, [(i, i ^ bits) for i in range(lax.axis_size(axis))])

    def share(name, g):
        for m in range(1, gx):
            values[name, g, m] = swap(values[name, g, m], "gx", m)

    def pass_on(g, which=None):
        for m in range(gx) if which is None else which:
            values["other", g, m] = swap(values["right", g, m], "gy", 1)

    def project_right(g):
        names = ("1d", "1u", "2d", "2u", "3", "r")
        arrays = [values["own", g, p] for p in range(2)] + [values[name, g] for name in names]
        slots = (
            ((0, (0, 1)), (1, (2, 3))),
            ((2, (0, 1)), (3, (2, 3))),
            ((4, (0, 1)), (5, (2, 3))),
            ((6, (0, 3)), (7, (1, 2))),
        )
        mask = right_mask[:, g * size : (g + 1) * size]
        outs = project(plane, slots, arrays, mask, right_weight, right_gain, gx, False)
        values.update({("right", g, m): outs[m] for m in range(gx)})

    def project_left(g):
        names = ("1d", "1u", "2d", "2u", "3", "l", "t")
        arrays = [values["own", g, p] for p in range(2)] + [values[name, g] for name in names]
        slots = (
            ((0, (0, 2)), (1, (1, 3))),
            ((2, (0, 2)), (3, (1, 3))),
            ((4, (0,)), (8, (1, 2)), (5, (3,))),
            ((6, (0, 3)), (7, (1, 2))),
        )
        mask = left_mask[:, g * size : (g + 1) * size]
        outs = project(plane, slots, arrays, mask, left_weight, left_gain, gx, True)
        values.update({("left", g, m): outs[m] for m in range(gx)})
        values["normed", g] = outs[gx]

    target = (((x // blocks) ^ y) * blocks + x % blocks) ^ jnp.arange(gx)
    target = target.astype(jnp.int32)

    def multiply(group):
        rights = [values[key, c, m] for key in ("right", "other") for c in range(CHUNKS) for m in range(gx)]
        lefts = [values["left", g, m] for g in group for m in range(gx)]
        outs = product(target, lefts, rights, gx, 4)
        for i, g in enumerate(group):
            values.update({("mixed", g, m): outs[i * gx + m] for m in range(gx)})

    def complete(g):
        mixed = [values["mixed", g, m] for m in range(gx)]
        outs = finish(mixed, values["normed", g], 0, out_weight, gate_weight, mix_gain, gz)
        values.update({("out", g, q): outs[q] for q in range(gz)})
        for q in range(1, gz):
            values["out", g, q] = swap(outs[q], "gz", q)

    def cut(g):
        for p in range(2):
            values["own", g, p] = values["tiles"][:, :, p, g * size : (g + 1) * size]
        values["side", g] = jnp.where(z < 2, values["own", g, 0], values["own", g, 1])

    values["tiles"] = tiles
    values.update({("held", i): array for i, array in enumerate(held)})
    cut(0)
    waits = ["tiles"]
    for e, messages in enumerate(EVENTS):
        keys = [key for message in EVENTS[e - 2] for key in results(message)] if e >= 2 else []
        keys += [key for message in messages for key in sources(message)]
        sync(*keys, *waits)
        waits = []
        for name, g in AHEAD.get(e, ()):
            (project_right if name == "right" else project_left)(g)
            share(name, g)
            keys = [(name, g, 0)] + [key for message in messages for key in sources(message)]
            sync(*keys)
        for message in messages:
            start(message)
        if e == 0:
            for g in range(1, CHUNKS):
                cut(g)
            waits = [("held", i) for i in range(len(held))]
        if e == 1:
            rows_held = [values["held", i] for i in range(len(held) - 1)] + [values["held", len(held) - 1][None]]
            mine = jnp.concatenate([w.astype(F32) for w in rows_held], axis=0)
            every = jnp.stack([mine] + [swap(mine, "gz", q) for q in range(1, gz)])
            depth = channels * gz
            row_order, col_order = jnp.asarray(ROW_ORDER)[z], jnp.asarray(COL_ORDER)[z]
            head_order = x ^ jnp.arange(gx)
            by_head = jnp.take(every, head_order ^ z, axis=0)

            def columns(blocks_of, i):
                part = blocks_of[:, i * depth : (i + 1) * depth]
                return jnp.swapaxes(part, 1, 2).reshape(-1, depth).astype(BF16)

            def lanes(vector):
                return jnp.broadcast_to(vector[:, None], (vector.shape[0], LANES))

            def pair_weight(gate, linear, order):
                return block_order(jnp.concatenate([columns(by_head, gate), columns(by_head, linear)]), order, 1)

            left_weight, right_weight = pair_weight(0, 1, row_order), pair_weight(2, 3, col_order)
            gate_weight = block_order(columns(every, 4), row_order, 1)
            out_weight = block_order(columns(every, 5), head_order, 1)
            left_gain, right_gain = (lanes(block_order(in_gain, order, 0)) for order in (row_order, col_order))
            mix_gain = lanes(by_head[:, -1].reshape(-1))
        for name, g in TASKS.get(e, ()):
            if name == "pass":
                pass_on(g)
            elif name == "early":
                pass_on(g, range(1))
            else:
                (project_right if name == "right" else project_left)(g)
                share(name, g)
                waits.append((name, g, 0))
        for name, g in TASKS.get(e + 1, ()):
            if name == "pass":
                waits += [("right", g, m) for m in range(gx)]
        for name, g in TASKS.get(e - 1, ()):
            if name == "pass":
                waits += [("other", g, m) for m in range(gx)]
        for name, g in TASKS.get(e - 3, ()):
            if name == "left":
                waits += [("left", g, m) for m in range(gx)]

    last = CHUNKS - 1
    sync(*waits, *[key for event in EVENTS[-2:] for message in event for key in results(message)])
    project_left(last)
    sync(("left", last, 0), *[("right", last - 1, m) for m in range(gx)])
    pass_on(last - 1)
    sync(("right", last, 1), *[("other", last - 1, m) for m in range(gx)])
    pass_on(last, range(1, 2))
    sync(("other", last, 1), *[("right", last, m) for m in range(2, gx)])
    pass_on(last, range(2, gx))
    previous = None
    for step, g in TAIL:
        needs = {"multiply": ["left"], "complete": ["mixed"], "share": ["left"]}[step]
        group = g if step == "multiply" else (g,)
        keys = [(name, c, m) for name in needs for c in group for m in range(gx)]
        sync(*keys, *([previous] if previous else []))
        if step == "multiply":
            multiply(group)
            previous = ("mixed", group[0], 0)
            for c in group:
                share("mixed", c)
        elif step == "share":
            share("left", g)
        else:
            complete(g)
            previous = ("out", g, 0)
    update = None
    for g in range(0, CHUNKS):
        update = assemble(plane, [values["out", g, q] for q in range(gz)], gz, g, CHUNKS, update)
    return update.reshape(pair.shape)


def plain_local(
    pair,
    pair_mask,
    in_gain,
    w_left,
    w_left_gate,
    w_right,
    w_right_gate,
    w_out_gate,
    out_gain,
    w_out,
):
    gathered = lax.all_gather(pair, "gz", axis=0, tiled=True).astype(F32)
    average = jnp.mean(gathered, axis=0)
    centered = gathered - average
    spread = jnp.mean(jnp.square(centered), axis=0)
    normed = (centered * lax.rsqrt(spread + epsilon) * in_gain[:, None, None]).astype(BF16)
    mask_float = pair_mask.astype(F32)[None]

    def project_all(weight):
        return jnp.einsum("cik,ch->hik", normed, weight, preferred_element_type=F32)

    left_rows = (mask_float * jax.nn.sigmoid(project_all(w_left_gate)) * project_all(w_left)).astype(BF16)
    right_rows = (mask_float * jax.nn.sigmoid(project_all(w_right_gate)) * project_all(w_right)).astype(BF16)
    out_gate = jax.nn.sigmoid(jnp.einsum("cij,cd->dij", normed, w_out_gate, preferred_element_type=F32))
    left_group, right_group = (
        lax.all_to_all(left_rows, "gx", split_axis=0, concat_axis=2, tiled=True),
        lax.all_to_all(right_rows, "gx", split_axis=0, concat_axis=2, tiled=True),
    )
    full_product = lax.dot_general(
        left_group,
        lax.all_gather(right_group, "gy", axis=1, tiled=True),
        (((2,), (2,)), ((0,), (0,))),
        preferred_element_type=F32,
    )
    mixed_sum = lax.all_to_all(full_product, "gx", split_axis=2, concat_axis=0, tiled=True)
    channel_count = lax.axis_size("gz") * mixed_sum.shape[0]
    mix_average = lax.psum(jnp.sum(mixed_sum, axis=0), "gz") / channel_count
    mix_centered = mixed_sum - mix_average
    mix_spread = lax.psum(jnp.sum(jnp.square(mix_centered), axis=0), "gz") / channel_count
    local_mix = (mix_centered * lax.rsqrt(mix_spread + epsilon) * out_gain[:, None, None]).astype(BF16)
    normed_mix = lax.all_gather(local_mix, "gz", axis=0, tiled=True)
    projected = jnp.einsum("hij,hd->dij", normed_mix, w_out, preferred_element_type=F32)
    return (out_gate * projected).astype(BF16)


def solution(mesh):
    placed = (
        P("gz", "gy", "gx"),
        P("gy", "gx"),
        P(),
        P(None, "gz"),
        P(None, "gz"),
        P(None, "gz"),
        P(None, "gz"),
        P(None, "gz"),
        P("gz"),
        P(None, "gz"),
    )
    fits = mesh.shape["gx"] == 4 and mesh.shape["gy"] == 2 and mesh.shape["gz"] == 4

    def step(*args):
        return local(*args) if fits else plain_local(*args)

    step = jax.shard_map(step, mesh=mesh, in_specs=placed, out_specs=P("gz", "gy", "gx"), check_vma=False)
    return step
```
